16 devices in a mesh: dp: 2 (over z), tp: 8 (over y, x, core).
Axes of the slice: x: 2, y: 2, z: 2, core: 2. Of those that a mesh axis runs over, the one named last changes fastest.
Arguments:
- x_in: bfloat16 [3, 2, 8, 512, 2048], P(None, None, 'dp')
- u_pre: bfloat16 [3, 2, 8, 512, 8192], P(None, None, 'dp', None, 'tp')
- w_up: bfloat16 [3, 2048, 8192], P(None, None, 'tp')
- w_down: bfloat16 [3, 8192, 2048], P(None, 'tp')
- d_out: bfloat16 [2, 8, 512, 2048], P(None, 'dp')
- noise_up: float32 [3, 2048, 8192], P(None, 'dp', 'tp')
- noise_down: float32 [3, 8192, 2048], P(None, 'tp', 'dp')
- clip_norm: float32 [1], replicated
- noise_mult: float32 [1], replicated
Outputs:
- output 1: float32 [3, 2048, 8192], P(None, 'dp', 'tp')
- output 2: float32 [3, 8192, 2048], P(None, 'tp', 'dp')
- output 3: bfloat16 [2, 8, 512, 2048], P(None, 'dp')
All inputs are finite; a program needn't handle non-finite values.
Results may differ from the reference program's by a relative error of at most 0.0169904.
Values are sent between devices in bfloat16 or wider.
A program may use at most 1 GiB of HBM per device.

```python
import math
import jax
import jax.numpy as jnp
from jax import lax

LAYERS = 3
MICRO = 2
GLOBAL_BATCH = 8
SEQ_LEN = 512
D_MODEL = 2048
D_FF = 8192

EXAMPLES = MICRO * GLOBAL_BATCH


def setup_inputs(seed: int = 0) -> dict:
    base_key = jax.random.key(seed)
    key_list = jax.random.split(base_key, 10)
    act_shape = (LAYERS, MICRO, GLOBAL_BATCH, SEQ_LEN)
    x_in = jax.random.normal(key_list[0], act_shape + (D_MODEL,), jnp.float32).astype(jnp.bfloat16)
    u_pre = jax.random.normal(key_list[1], act_shape + (D_FF,), jnp.float32).astype(jnp.bfloat16)
    w_up = (jax.random.normal(key_list[2], (LAYERS, D_MODEL, D_FF), jnp.float32) * D_MODEL ** -0.5).astype(jnp.bfloat16)
    w_down = (jax.random.normal(key_list[3], (LAYERS, D_FF, D_MODEL), jnp.float32) * D_FF ** -0.5).astype(jnp.bfloat16)
    log_scale = jax.random.uniform(key_list[4], (MICRO, GLOBAL_BATCH, 1, 1), jnp.float32, math.log(0.5), math.log(16.0))
    d_out = (jax.random.normal(key_list[5], (MICRO, GLOBAL_BATCH, SEQ_LEN, D_MODEL), jnp.float32) * jnp.exp(log_scale)).astype(jnp.bfloat16)
    noise_up = jax.random.normal(key_list[6], (LAYERS, D_MODEL, D_FF), jnp.float32)
    noise_down = jax.random.normal(key_list[7], (LAYERS, D_FF, D_MODEL), jnp.float32)
    clip_norm = jax.random.uniform(key_list[8], (1,), jnp.float32, 0.6, 1.0) * math.sqrt(LAYERS * SEQ_LEN * D_MODEL * D_FF)
    noise_mult = jnp.exp(jax.random.uniform(key_list[9], (1,), jnp.float32, math.log(0.08), math.log(0.75))) * math.sqrt(EXAMPLES / (2.0 * LAYERS * D_MODEL * D_FF))
    return {"x_in": x_in, "u_pre": u_pre, "w_up": w_up, "w_down": w_down, "d_out": d_out, "noise_up": noise_up, "noise_down": noise_down, "clip_norm": clip_norm, "noise_mult": noise_mult}


def reference(x_in, u_pre, w_up, w_down, d_out, noise_up, noise_down, clip_norm, noise_mult):
    x_rows = x_in.reshape(LAYERS, EXAMPLES, SEQ_LEN, D_MODEL)
    u_rows = u_pre.reshape(LAYERS, EXAMPLES, SEQ_LEN, D_FF)
    top_cot = d_out.reshape(EXAMPLES, SEQ_LEN, D_MODEL)

    def layer_step(carry_in, layer_in):
        grad_cot, norm_vec = carry_in
        x_layer, u_layer, w_first, w_second = layer_in
        w_first_t = w_first.T
        w_second_t = w_second.T

        def one_example(example):
            x_ex, u_ex, cot_ex = example
            gelu_out, gelu_vjp = jax.vjp(jax.nn.gelu, u_ex.astype(jnp.float32))
            hidden = gelu_out.astype(jnp.bfloat16)
            d_act = jnp.dot(cot_ex, w_second_t, preferred_element_type=jnp.float32)
            d_hid = gelu_vjp(d_act)[0].astype(jnp.bfloat16)
            back_prop = jnp.dot(d_hid, w_first_t, preferred_element_type=jnp.float32)
            new_cot = (cot_ex.astype(jnp.float32) + back_prop).astype(jnp.bfloat16)
            gram_term = jnp.sum(jnp.dot(hidden, hidden.T, preferred_element_type=jnp.float32) * jnp.dot(cot_ex, cot_ex.T, preferred_element_type=jnp.float32))
            gram_term = gram_term + jnp.sum(jnp.dot(x_ex, x_ex.T, preferred_element_type=jnp.float32) * jnp.dot(d_hid, d_hid.T, preferred_element_type=jnp.float32))
            return new_cot, gram_term, hidden, d_hid

        new_cot, gram_add, hid_layer, dhid_layer = lax.map(one_example, (x_layer, u_layer, grad_cot))
        return (new_cot, norm_vec + gram_add), (hid_layer, dhid_layer, grad_cot)

    start_carry = (top_cot, jnp.zeros((EXAMPLES,), jnp.float32))
    (d_in, norm_vec), (hid_all, dhid_all, cot_all) = lax.scan(layer_step, start_carry, (x_rows, u_rows, w_up, w_down), reverse=True)
    clip_fac = jnp.minimum(1.0, clip_norm[0] / jnp.sqrt(norm_vec))
    scale_col = clip_fac[:, None, None]

    def weight_grads(layer_in):
        x_layer, hidden, d_hid, grad_cot = layer_in
        scaled_dh = (d_hid.astype(jnp.float32) * scale_col).astype(jnp.bfloat16)
        scaled_cot = (grad_cot.astype(jnp.float32) * scale_col).astype(jnp.bfloat16)
        up_grad = jnp.dot(x_layer.reshape(-1, D_MODEL).T, scaled_dh.reshape(-1, D_FF), preferred_element_type=jnp.float32)
        down_grad = jnp.dot(hidden.reshape(-1, D_FF).T, scaled_cot.reshape(-1, D_MODEL), preferred_element_type=jnp.float32)
        return up_grad, down_grad

    up_sum, down_sum = lax.map(weight_grads, (x_rows, hid_all, dhid_all, cot_all))
    noise_scale = noise_mult[0] * clip_norm[0]
    grad_up = (up_sum + noise_scale * noise_up) / EXAMPLES
    grad_down = (down_sum + noise_scale * noise_down) / EXAMPLES
    return grad_up, grad_down, d_in.reshape(MICRO, GLOBAL_BATCH, SEQ_LEN, D_MODEL)
```

```python
import functools
import math

import jax
import jax.numpy as jnp
from jax import lax
from jax.experimental import pallas as pl
from jax.experimental.pallas import tpu as pltpu
from jax.sharding import PartitionSpec as P


PIECE = 256
HALF = 1024
PER_CHUNK = 2
TANH_SCALE = math.sqrt(2.0 / math.pi)
TANH_CUBE = 0.044715

NT = (((1,), (1,)), ((), ()))
TN = (((0,), (0,)), ((), ()))


def dot(lhs, rhs, dims):
    return lax.dot_general(lhs, rhs, dims, preferred_element_type=jnp.float32)


def piece_of(me, r1, r2, rc, x_first):
    bits = (r2 * 4 + r1 * 2 + rc) if x_first else (r1 * 4 + r2 * 2 + rc)
    return me ^ bits


def backward_kernel(x_first, from_slots, me_ref, *refs):
    if from_slots:
        own, first, core_own, core_first, u_ref, w1_ref, w2_ref, h_ref, dh_ref, keep_ref, send_ref, dz_ref = refs
    else:
        dz_in, u_ref, w1_ref, w2_ref, h_ref, dh_ref, keep_ref, send_ref = refs
    me = me_ref[0]
    if from_slots:
        for rc, r1, slots in ((0, 0, own), (0, 1, first), (1, 0, core_own), (1, 1, core_first)):
            for r2 in range(2):
                start = pl.multiple_of(piece_of(me, r1, r2, rc, x_first) * PIECE, PIECE)
                dz_ref[:, pl.ds(start, PIECE)] = slots[r2]
        cot = dz_ref
    else:
        cot = dz_in
    width = 256
    for j in range(u_ref.shape[-1] // width):
        cols = slice(j * width, (j + 1) * width)
        d_act = dot(cot[...], w2_ref[cols, :], NT)
        u = u_ref[:, cols].astype(jnp.float32)
        u_sq = u * u
        t = jnp.tanh(TANH_SCALE * (u + TANH_CUBE * (u_sq * u)))
        cdf = 0.5 * (1.0 + t)
        slope = cdf + (0.5 * TANH_SCALE) * (1.0 - t * t) * (u * (1.0 + (3.0 * TANH_CUBE) * u_sq))
        h_ref[:, cols] = (u * cdf).astype(jnp.bfloat16)
        dh_ref[:, cols] = (slope * d_act).astype(jnp.bfloat16)
    for rc, out in ((1, send_ref), (0, keep_ref)):
        for r1 in range(2):
            for r2 in range(2):
                start = pl.multiple_of(piece_of(me, r1, r2, rc, x_first) * PIECE, PIECE)
                out[r1, r2] = dot(dh_ref[...], w1_ref[pl.ds(start, PIECE), :], NT).astype(jnp.bfloat16)


def backward_chunk(layer, micro, first_ex, x_first, me, dz_inputs, u_pre, w_up, w_down):
    rows = PER_CHUNK * 512
    hid, model = u_pre.shape[-1], w_up.shape[1]
    from_slots = isinstance(dz_inputs, tuple)
    slot_spec = pl.BlockSpec((2, 512, PIECE), lambda e, m: (0, e, 0))
    if from_slots:
        dz_specs = [slot_spec] * 4
    else:
        dz_specs = [pl.BlockSpec((None, None, 512, model), lambda e, m: (micro, first_ex + e, 0, 0))]
        dz_inputs = (dz_inputs,)
    part_spec = pl.BlockSpec((2, 2, 512, PIECE), lambda e, m: (0, 0, e, 0))
    part_shape = jax.ShapeDtypeStruct((2, 2, rows, PIECE), jnp.bfloat16)
    act_spec = pl.BlockSpec((512, hid), lambda e, m: (e, 0))
    act_shape = jax.ShapeDtypeStruct((rows, hid), jnp.bfloat16)
    out_specs = [act_spec, act_spec, part_spec, part_spec]
    out_shape = [act_shape, act_shape, part_shape, part_shape]
    if from_slots:
        out_specs.append(pl.BlockSpec((512, model), lambda e, m: (e, 0)))
        out_shape.append(jax.ShapeDtypeStruct((rows, model), jnp.bfloat16))
    return pl.pallas_call(
        functools.partial(backward_kernel, x_first, from_slots),
        grid_spec=pltpu.PrefetchScalarGridSpec(
            num_scalar_prefetch=1,
            grid=(PER_CHUNK,),
            in_specs=dz_specs
            + [
                pl.BlockSpec((None, None, None, 512, hid), lambda e, m: (layer, micro, first_ex + e, 0, 0)),
                pl.BlockSpec((None, model, hid), lambda e, m: (layer, 0, 0)),
                pl.BlockSpec((None, hid, model), lambda e, m: (layer, 0, 0)),
            ],
            out_specs=out_specs,
        ),
        out_shape=out_shape,
        compiler_params=pltpu.CompilerParams(dimension_semantics=("arbitrary",)),
        cost_estimate=pl.CostEstimate(flops=4 * rows * hid * model, bytes_accessed=20 << 20, transcendentals=rows * hid),
        name=f"backward_{layer}_{micro}_{first_ex}",
    )(me, *dz_inputs, u_pre, w_up, w_down)


def norm_kernel(h_ref, dh_ref, dz_ref, x_ref, out_ref):
    total = jnp.zeros((256, 256), jnp.float32)
    for left, right in ((h_ref, dz_ref), (dh_ref, x_ref)):
        a = dot(left[...], left[:256, :], NT)
        b = dot(right[...], right[:256, :], NT)
        prod = a * b
        total += prod[:256] + 2.0 * prod[256:]
        total += dot(left[256:, :], left[256:, :], NT) * dot(right[256:, :], right[256:, :], NT)
    out_ref[...] = jnp.sum(total.reshape(32, 8, 256), axis=0)


def norm_chunk(layer, micro, first_ex, hidden, d_hid, cot, x_in):
    hid, model = hidden.shape[1], x_in.shape[-1]
    act_spec = pl.BlockSpec((512, hid), lambda e: (e, 0))
    if cot.ndim == 4:
        cot_spec = pl.BlockSpec((None, None, 512, model), lambda e: (micro, first_ex + e, 0, 0))
    else:
        cot_spec = pl.BlockSpec((512, model), lambda e: (e, 0))
    return pl.pallas_call(
        norm_kernel,
        grid=(PER_CHUNK,),
        in_specs=[
            act_spec,
            act_spec,
            cot_spec,
            pl.BlockSpec((None, None, None, 512, model), lambda e: (layer, micro, first_ex + e, 0, 0)),
        ],
        out_specs=pl.BlockSpec((None, 8, 256), lambda e: (e, 0, 0)),
        out_shape=jax.ShapeDtypeStruct((PER_CHUNK, 8, 256), jnp.float32),
        compiler_params=pltpu.CompilerParams(dimension_semantics=("arbitrary",)),
        cost_estimate=pl.CostEstimate(
            flops=3 * PER_CHUNK * 512 * 512 * (hid + model), bytes_accessed=PER_CHUNK * 6 << 20, transcendentals=0
        ),
        name=f"norm_{layer}_{micro}_{first_ex}",
    )(hidden, d_hid, cot, x_in)


def grad_kernel(up, n_chunks, with_noise, half_ref, clip_ref, *refs):
    if with_noise:
        scale_ref, refs = refs[0], refs[1:]
    lhs, rhs = refs[:-1][: (1 if up else n_chunks)], refs[:-1][(1 if up else n_chunks) :]
    if with_noise:
        noise_ref, rhs = rhs[-1], rhs[:-1]
    out_ref = refs[-1]
    step = pl.program_id(0)

    @pl.when(step == 0)
    def _():
        out_ref[...] = scale_ref[0] * noise_ref[...] if with_noise else jnp.zeros_like(out_ref)

    clip = clip_ref[step]
    for k in range(n_chunks):

        @pl.when(step // PER_CHUNK == k)
        def _(k=k):
            a = lhs[min(k, len(lhs) - 1)]
            b = rhs[min(k, len(rhs) - 1)]
            scaled = (b[...].astype(jnp.float32) * clip).astype(jnp.bfloat16)
            for j in range(2):
                cols = slice(j * 512, (j + 1) * 512)
                out_ref[:, cols] += dot(a[...], scaled[:, cols], TN)


def weight_grad(up, layer, half, clip, lhs, rhs, noise=None, noise_scale=None):
    n_chunks = len(lhs) if not up else len(rhs)
    n_ex = n_chunks * PER_CHUNK

    def chunk_row(k):
        return lambda s, h: (jnp.clip(s - PER_CHUNK * k, 0, PER_CHUNK - 1), 0)

    def chunk_half(k):
        return lambda s, h: (jnp.clip(s - PER_CHUNK * k, 0, PER_CHUNK - 1), h[0])

    if up:
        lhs_specs = [pl.BlockSpec((None, None, None, 512, HALF), lambda s, h: (layer, s // 4, s % 4, 0, h[0]))]
        rhs_specs = [pl.BlockSpec((512, 1024), chunk_row(k)) for k in range(n_chunks)]
        lhs = (lhs,)
    else:
        lhs_specs = [pl.BlockSpec((512, 1024), chunk_row(k)) for k in range(n_chunks)]
        if isinstance(rhs, tuple):
            rhs_specs = [pl.BlockSpec((512, HALF), chunk_half(k)) for k in range(n_chunks)]
        else:
            rhs_specs = [pl.BlockSpec((None, None, 512, HALF), lambda s, h: (s // 4, s % 4, 0, h[0]))]
            rhs = (rhs,)
    extra, extra_specs, lead, lead_specs = (), [], (), []
    if noise is not None:
        extra = (noise,)
        extra_specs = [pl.BlockSpec((None, 1024, 1024), lambda s, h: (layer, 0, 0))]
        lead = (noise_scale,)
        lead_specs = [pl.BlockSpec(memory_space=pltpu.SMEM)]
    return pl.pallas_call(
        functools.partial(grad_kernel, up, n_chunks, noise is not None),
        grid_spec=pltpu.PrefetchScalarGridSpec(
            num_scalar_prefetch=1,
            grid=(n_ex,),
            in_specs=[pl.BlockSpec(memory_space=pltpu.SMEM)] + lead_specs + lhs_specs + rhs_specs + extra_specs,
            out_specs=pl.BlockSpec((1024, 1024), lambda s, h: (0, 0)),
        ),
        out_shape=jax.ShapeDtypeStruct((1024, 1024), jnp.float32),
        compiler_params=pltpu.CompilerParams(dimension_semantics=("arbitrary",)),
        cost_estimate=pl.CostEstimate(flops=2 * n_ex * 512 * 1024 * 1024, bytes_accessed=24 << 20, transcendentals=0),
        name=f"grad_{'up' if up else 'down'}_{layer}_{'own' if noise is not None else 'other'}",
    )(half, clip, *lead, *lhs, *rhs, *extra)


def finish_kernel(inv, own_ref, got_ref, *refs):
    refs[-1][...] = (own_ref[...] + got_ref[...]) * inv


def finish_grad(layer, n_layers, examples, own, got, buffer):
    spec = pl.BlockSpec((256, 1024), lambda i: (i, 0))
    operands, in_specs, aliases = (own, got), [spec, spec], {}
    if buffer is not None:
        operands, in_specs, aliases = (own, got, buffer), [spec, spec, pl.BlockSpec(memory_space=pl.ANY)], {2: 0}
    return pl.pallas_call(
        functools.partial(finish_kernel, 1.0 / examples),
        grid=(4,),
        in_specs=in_specs,
        out_specs=pl.BlockSpec((None, 256, 1024), lambda i: (layer, i, 0)),
        out_shape=jax.ShapeDtypeStruct((n_layers, 1024, 1024), jnp.float32),
        input_output_aliases=aliases,
        compiler_params=pltpu.CompilerParams(dimension_semantics=("arbitrary",)),
        cost_estimate=pl.CostEstimate(flops=12 << 20, bytes_accessed=12 << 20, transcendentals=0),
        name=f"finish_{layer}",
    )(*operands)


def join_kernel(orders, me_ref, *refs):
    out_ref = refs[-1]
    step = pl.program_id(0)
    for k, x_first in enumerate(orders):

        @pl.when(step // PER_CHUNK == k)
        def _(k=k, x_first=x_first):
            own, first, core_own, core_first = refs[4 * k : 4 * k + 4]
            for rc, r1, slots in ((0, 0, own), (0, 1, first), (1, 0, core_own), (1, 1, core_first)):
                for r2 in range(2):
                    start = pl.multiple_of(piece_of(me_ref[0], r1, r2, rc, x_first) * PIECE, PIECE)
                    out_ref[:, pl.ds(start, PIECE)] = slots[r2]


def join_slots(me, orders, chunks, shape):
    def spec(k):
        return pl.BlockSpec((2, 512, PIECE), lambda s, m: (0, jnp.clip(s - PER_CHUNK * k, 0, PER_CHUNK - 1), 0))

    return pl.pallas_call(
        functools.partial(join_kernel, orders),
        grid_spec=pltpu.PrefetchScalarGridSpec(
            num_scalar_prefetch=1,
            grid=(len(orders) * PER_CHUNK,),
            in_specs=[spec(k) for k in range(len(orders)) for _ in range(4)],
            out_specs=pl.BlockSpec((None, None, 512, shape[-1]), lambda s, m: (s // 4, s % 4, 0, 0)),
        ),
        out_shape=jax.ShapeDtypeStruct(shape, jnp.bfloat16),
        compiler_params=pltpu.CompilerParams(dimension_semantics=("arbitrary",)),
        cost_estimate=pl.CostEstimate(flops=32 << 20, bytes_accessed=32 << 20, transcendentals=0),
        name="join_d_in",
    )(me, *[s for chunk in chunks for s in chunk])


def solution(mesh):
    dp_size, tp_size = mesh.shape["dp"], mesh.shape["tp"]
    CORE, X, Y = 1, 2, 4

    def swap(value, mask):
        return lax.ppermute(value, "tp", [(i, i ^ mask) for i in range(tp_size)])

    def add(a, b):
        return (a.astype(jnp.float32) + b.astype(jnp.float32)).astype(jnp.bfloat16)

    def sum_over_tp(keep, send, cot_piece, x_first):
        one, two = (X, Y) if x_first else (Y, X)
        got = swap(send, CORE)
        got = (swap(add(keep[1], got[1]), one), add(keep[0], got[0]))
        pair = got[0]
        kept = got[1]
        last = swap(add(kept[1], pair[1]), two)
        mine = add(kept[0], pair[0])
        piece = (cot_piece.astype(jnp.float32) + (mine.astype(jnp.float32) + last.astype(jnp.float32))).astype(jnp.bfloat16)
        own = jnp.stack([piece, swap(piece, two)])
        first = swap(own, one)
        return piece, (own, first, swap(own, CORE), swap(first, CORE))

    def local_pass(x_in, u_pre, w_up, w_down, d_out, noise_up, noise_down, clip_norm, noise_mult):
        n_layers = x_in.shape[0]
        micro, per_micro = d_out.shape[:2]
        examples = micro * per_micro * dp_size
        me = lax.axis_index("tp").astype(jnp.int32)
        my_dp = lax.axis_index("dp").astype(jnp.int32)
        me_arr = me.reshape(1)
        chunks = [(m, e) for m in range(micro) for e in range(0, per_micro, PER_CHUNK)]
        orders = [k % 2 == 0 for k in range(len(chunks))]
        cots = [d_out] * len(chunks)
        pieces = [
            lax.dynamic_slice_in_dim(d_out[m, e : e + PER_CHUNK].reshape(-1, d_out.shape[-1]), me * PIECE, PIECE, 1)
            for m, e in chunks
        ]
        norm_part = [0.0] * len(chunks)
        saved = [None] * n_layers
        for layer in reversed(range(n_layers)):
            hids, dhids, full = [], [], []
            for k, (m, e) in enumerate(chunks):
                outs = backward_chunk(layer, m, e, orders[k], me_arr, cots[k], u_pre, w_up, w_down)
                hidden, d_hid, keep, send = outs[:4]
                cot = outs[4] if len(outs) == 5 else d_out
                norm_part[k] += jnp.sum(norm_chunk(layer, m, e, hidden, d_hid, cot, x_in), axis=(1, 2))
                pieces[k], cots[k] = sum_over_tp(keep, send, pieces[k], orders[k])
                hids.append(hidden)
                dhids.append(d_hid)
                full.append(cot)
            saved[layer] = (tuple(hids), tuple(dhids), d_out if layer == n_layers - 1 else tuple(full))
        d_in = join_slots(me_arr, orders, cots, d_out.shape)
        norm_vec = lax.psum(jnp.concatenate(norm_part), "tp")
        clip = jnp.minimum(1.0, clip_norm[0] / jnp.sqrt(norm_vec))
        noise_scale = (noise_mult[0] * clip_norm[0]).reshape(1)
        own_half, other_half = my_dp.reshape(1), (1 - my_dp).reshape(1)
        swap_dp = [(i, 1 - i) for i in range(dp_size)]
        up, down = None, None
        got = []
        for layer in reversed(range(n_layers)):
            hids, dhids, full = saved[layer]
            got.append(lax.ppermute(weight_grad(True, layer, other_half, clip, x_in, dhids), "dp", swap_dp))
            got.append(lax.ppermute(weight_grad(False, layer, other_half, clip, hids, full), "dp", swap_dp))
        for i, layer in enumerate(reversed(range(n_layers))):
            hids, dhids, full = saved[layer]
            own_up = weight_grad(True, layer, own_half, clip, x_in, dhids, noise_up, noise_scale)
            own_down = weight_grad(False, layer, own_half, clip, hids, full, noise_down, noise_scale)
            up = finish_grad(layer, n_layers, examples, own_up, got[2 * i], up)
            down = finish_grad(layer, n_layers, examples, own_down, got[2 * i + 1], down)
        return up, down, d_in

    in_specs = (P(None, None, "dp", None, None), P(None, None, "dp", None, "tp"), P(None, None, "tp"), P(None, "tp", None), P(None, "dp", None, None), P(None, "dp", "tp"), P(None, "tp", "dp"), P(), P())
    out_specs = (P(None, "dp", "tp"), P(None, "tp", "dp"), P(None, "dp", None, None))
    return jax.shard_map(local_pass, mesh=mesh, in_specs=in_specs, out_specs=out_specs, check_vma=False)
```

```python
import functools
import math

import jax
import jax.numpy as jnp
from jax import lax
from jax.experimental import pallas as pl
from jax.experimental.pallas import tpu as pltpu
from jax.sharding import PartitionSpec as P


PIECE = 256
HALF = 1024
PER_CHUNK = 2
TANH_SCALE = math.sqrt(2.0 / math.pi)
TANH_CUBE = 0.044715

NT = (((1,), (1,)), ((), ()))
TN = (((0,), (0,)), ((), ()))


def dot(lhs, rhs, dims):
    return lax.dot_general(lhs, rhs, dims, preferred_element_type=jnp.float32)


def piece_of(me, r1, r2, rc, x_first):
    bits = (r2 * 4 + r1 * 2 + rc) if x_first else (r1 * 4 + r2 * 2 + rc)
    return me ^ bits


def backward_kernel(layer, micro, first_ex, x_first, from_slots, me_ref, *refs):
    *refs, w1, w2, x_buf, w1_sem, w2_sem, x_sem = refs
    if from_slots:
        own, first, core_own, core_first, norm_in, u_ref, w1_hbm, w2_hbm, x_hbm = refs[:9]
        h_ref, dh_ref, keep_ref, send_ref, norm_ref, dz_ref = refs[9:]
    else:
        dz_in, u_ref, w1_hbm, w2_hbm, x_hbm, h_ref, dh_ref, keep_ref, send_ref, norm_ref, piece_ref = refs
    me = me_ref[0]
    step = pl.program_id(0)
    slots = [(rc, r1, r2) for rc in (1, 0) for r1 in range(2) for r2 in range(2)]
    hid = u_ref.shape[-1]

    def rows_of(rc, r1, r2):
        return pl.ds(pl.multiple_of(piece_of(me, r1, r2, rc, x_first) * PIECE, PIECE), PIECE)

    def w2_copy(i):
        rows = pl.ds(i * (hid // 2), hid // 2)
        return pltpu.make_async_copy(w2_hbm.at[layer, rows, :], w2.at[rows, :], w2_sem.at[i])

    def w1_copy(i):
        return pltpu.make_async_copy(w1_hbm.at[layer, rows_of(*slots[i]), :], w1.at[i], w1_sem.at[i])

    def x_copy():
        return pltpu.make_async_copy(x_hbm.at[layer, micro, first_ex + step], x_buf, x_sem)

    @pl.when(step == 0)
    def _():
        for i in range(2):
            w2_copy(i).start()
        for i in range(8):
            w1_copy(i).start()

    x_copy().start()
    if from_slots:
        for rc, r1, slot in ((0, 0, own), (0, 1, first), (1, 0, core_own), (1, 1, core_first)):
            for r2 in range(2):
                dz_ref[:, rows_of(rc, r1, r2)] = slot[r2]
        cot = dz_ref
    else:
        cot = dz_in
        piece_ref[...] = dz_in[:, pl.ds(pl.multiple_of(me * PIECE, PIECE), PIECE)]
    width = 256
    for j in range(hid // width):
        if j % 2 == 0:

            @pl.when(step == 0)
            def _(j=j):
                w2_copy(j // 2).wait()

        cols = slice(j * width, (j + 1) * width)
        d_act = dot(cot[...], w2[cols, :], NT)
        u = u_ref[:, cols].astype(jnp.float32)
        u_sq = u * u
        t = jnp.tanh(TANH_SCALE * (u + TANH_CUBE * (u_sq * u)))
        cdf = 0.5 * (1.0 + t)
        slope = cdf + (0.5 * TANH_SCALE) * (1.0 - t * t) * (u * (1.0 + (3.0 * TANH_CUBE) * u_sq))
        h_ref[:, cols] = (u * cdf).astype(jnp.bfloat16)
        dh_ref[:, cols] = (slope * d_act).astype(jnp.bfloat16)

    @pl.when(step == 0)
    def _():
        for i in range(8):
            w1_copy(i).wait()

    for i, (rc, r1, r2) in enumerate(slots):
        out = send_ref if rc else keep_ref
        out[r1, r2] = dot(dh_ref[...], w1[i], NT).astype(jnp.bfloat16)

    def gram_product(left, right):
        prod = dot(left[...], left[:256, :], NT) * dot(right[...], right[:256, :], NT)
        corner = dot(left[256:, :], left[256:, :], NT) * dot(right[256:, :], right[256:, :], NT)
        total = prod[:256] + 2.0 * prod[256:] + corner
        return jnp.sum(total.reshape(32, 8, 256), axis=0)

    norm = gram_product(h_ref, cot)
    x_copy().wait()
    norm += gram_product(dh_ref, x_buf)
    norm_ref[...] = norm_in[...] + norm if from_slots else norm


def backward_chunk(layer, micro, first_ex, x_first, me, dz_inputs, norm_in, x_in, u_pre, w_up, w_down):
    rows = PER_CHUNK * 512
    hid, model = u_pre.shape[-1], w_up.shape[1]
    from_slots = isinstance(dz_inputs, tuple)
    norm_spec = pl.BlockSpec((None, 8, 256), lambda e, m: (e, 0, 0))
    piece_spec = pl.BlockSpec((512, PIECE), lambda e, m: (e, 0))
    if from_slots:
        in_specs = [pl.BlockSpec((2, 512, PIECE), lambda e, m: (0, e, 0))] * 4 + [norm_spec]
        operands = (*dz_inputs, norm_in)
    else:
        in_specs = [pl.BlockSpec((None, None, 512, model), lambda e, m: (micro, first_ex + e, 0, 0))]
        operands = (dz_inputs,)
    part_spec = pl.BlockSpec((2, 2, 512, PIECE), lambda e, m: (0, 0, e, 0))
    part_shape = jax.ShapeDtypeStruct((2, 2, rows, PIECE), jnp.bfloat16)
    act_spec = pl.BlockSpec((512, hid), lambda e, m: (e, 0))
    act_shape = jax.ShapeDtypeStruct((rows, hid), jnp.bfloat16)
    last_cols = model if from_slots else PIECE
    any_spec = pl.BlockSpec(memory_space=pl.ANY)
    return pl.pallas_call(
        functools.partial(backward_kernel, layer, micro, first_ex, x_first, from_slots),
        grid_spec=pltpu.PrefetchScalarGridSpec(
            num_scalar_prefetch=1,
            grid=(PER_CHUNK,),
            in_specs=in_specs
            + [pl.BlockSpec((None, None, None, 512, hid), lambda e, m: (layer, micro, first_ex + e, 0, 0))]
            + [any_spec] * 3,
            out_specs=[act_spec, act_spec, part_spec, part_spec, norm_spec]
            + [pl.BlockSpec((512, last_cols), lambda e, m: (e, 0))],
            scratch_shapes=[
                pltpu.VMEM((8, PIECE, hid), jnp.bfloat16),
                pltpu.VMEM((hid, model), jnp.bfloat16),
                pltpu.VMEM((512, model), jnp.bfloat16),
                pltpu.SemaphoreType.DMA((8,)),
                pltpu.SemaphoreType.DMA((2,)),
                pltpu.SemaphoreType.DMA,
            ],
        ),
        out_shape=[act_shape, act_shape, part_shape, part_shape]
        + [jax.ShapeDtypeStruct((PER_CHUNK, 8, 256), jnp.float32), jax.ShapeDtypeStruct((rows, last_cols), jnp.bfloat16)],
        compiler_params=pltpu.CompilerParams(dimension_semantics=("arbitrary",)),
        cost_estimate=pl.CostEstimate(flops=6 * rows * hid * model, bytes_accessed=24 << 20, transcendentals=rows * hid),
    )(me, *operands, u_pre, w_up, w_down, x_in)


def grad_kernel(up, n_chunks, with_noise, half_ref, clip_ref, *refs):
    if with_noise:
        scale_ref, refs = refs[0], refs[1:]
    lhs, rhs = refs[:-1][: (1 if up else n_chunks)], refs[:-1][(1 if up else n_chunks) :]
    if with_noise:
        noise_ref, rhs = rhs[-1], rhs[:-1]
    out_ref = refs[-1]
    step = pl.program_id(0)

    @pl.when(step == 0)
    def _():
        out_ref[...] = scale_ref[0] * noise_ref[...] if with_noise else jnp.zeros_like(out_ref)

    clip = clip_ref[step]
    for k in range(n_chunks):

        @pl.when(step // PER_CHUNK == k)
        def _(k=k):
            a = lhs[min(k, len(lhs) - 1)]
            b = rhs[min(k, len(rhs) - 1)]
            scaled = (b[...].astype(jnp.float32) * clip).astype(jnp.bfloat16)
            for j in range(2):
                cols = slice(j * 512, (j + 1) * 512)
                out_ref[:, cols] += dot(a[...], scaled[:, cols], TN)


def weight_grad(up, layer, half, clip, lhs, rhs, noise=None, noise_scale=None):
    n_chunks = len(lhs) if not up else len(rhs)
    n_ex = n_chunks * PER_CHUNK

    def chunk_row(k):
        return lambda s, h: (jnp.clip(s - PER_CHUNK * k, 0, PER_CHUNK - 1), 0)

    def chunk_half(k):
        return lambda s, h: (jnp.clip(s - PER_CHUNK * k, 0, PER_CHUNK - 1), h[0])

    if up:
        lhs_specs = [pl.BlockSpec((None, None, None, 512, HALF), lambda s, h: (layer, s // 4, s % 4, 0, h[0]))]
        rhs_specs = [pl.BlockSpec((512, 1024), chunk_row(k)) for k in range(n_chunks)]
        lhs = (lhs,)
    else:
        lhs_specs = [pl.BlockSpec((512, 1024), chunk_row(k)) for k in range(n_chunks)]
        if isinstance(rhs, tuple):
            rhs_specs = [pl.BlockSpec((512, HALF), chunk_half(k)) for k in range(n_chunks)]
        else:
            rhs_specs = [pl.BlockSpec((None, None, 512, HALF), lambda s, h: (s // 4, s % 4, 0, h[0]))]
            rhs = (rhs,)
    extra, extra_specs, lead, lead_specs = (), [], (), []
    if noise is not None:
        extra = (noise,)
        extra_specs = [pl.BlockSpec((None, 1024, 1024), lambda s, h: (layer, 0, 0))]
        lead = (noise_scale,)
        lead_specs = [pl.BlockSpec(memory_space=pltpu.SMEM)]
    return pl.pallas_call(
        functools.partial(grad_kernel, up, n_chunks, noise is not None),
        grid_spec=pltpu.PrefetchScalarGridSpec(
            num_scalar_prefetch=1,
            grid=(n_ex,),
            in_specs=[pl.BlockSpec(memory_space=pltpu.SMEM)] + lead_specs + lhs_specs + rhs_specs + extra_specs,
            out_specs=pl.BlockSpec((1024, 1024), lambda s, h: (0, 0)),
        ),
        out_shape=jax.ShapeDtypeStruct((1024, 1024), jnp.float32),
        compiler_params=pltpu.CompilerParams(dimension_semantics=("arbitrary",)),
        cost_estimate=pl.CostEstimate(flops=2 * n_ex * 512 * 1024 * 1024, bytes_accessed=24 << 20, transcendentals=0),
    )(half, clip, *lead, *lhs, *rhs, *extra)


def finish_kernel(inv, own_ref, got_ref, *refs):
    refs[-1][...] = (own_ref[...] + got_ref[...]) * inv


def finish_grad(layer, n_layers, examples, own, got, buffer):
    spec = pl.BlockSpec((256, 1024), lambda i: (i, 0))
    operands, in_specs, aliases = (own, got), [spec, spec], {}
    if buffer is not None:
        operands, in_specs, aliases = (own, got, buffer), [spec, spec, pl.BlockSpec(memory_space=pl.ANY)], {2: 0}
    return pl.pallas_call(
        functools.partial(finish_kernel, 1.0 / examples),
        grid=(4,),
        in_specs=in_specs,
        out_specs=pl.BlockSpec((None, 256, 1024), lambda i: (layer, i, 0)),
        out_shape=jax.ShapeDtypeStruct((n_layers, 1024, 1024), jnp.float32),
        input_output_aliases=aliases,
        compiler_params=pltpu.CompilerParams(dimension_semantics=("arbitrary",)),
        cost_estimate=pl.CostEstimate(flops=12 << 20, bytes_accessed=12 << 20, transcendentals=0),
    )(*operands)


def join_kernel(orders, me_ref, *refs):
    out_ref = refs[-1]
    step = pl.program_id(0)
    for k, x_first in enumerate(orders):

        @pl.when(step // PER_CHUNK == k)
        def _(k=k, x_first=x_first):
            own, first, core_own, core_first = refs[4 * k : 4 * k + 4]
            for rc, r1, slots in ((0, 0, own), (0, 1, first), (1, 0, core_own), (1, 1, core_first)):
                for r2 in range(2):
                    start = pl.multiple_of(piece_of(me_ref[0], r1, r2, rc, x_first) * PIECE, PIECE)
                    out_ref[:, pl.ds(start, PIECE)] = slots[r2]


def join_slots(me, orders, chunks, shape):
    def spec(k):
        return pl.BlockSpec((2, 512, PIECE), lambda s, m: (0, jnp.clip(s - PER_CHUNK * k, 0, PER_CHUNK - 1), 0))

    return pl.pallas_call(
        functools.partial(join_kernel, orders),
        grid_spec=pltpu.PrefetchScalarGridSpec(
            num_scalar_prefetch=1,
            grid=(len(orders) * PER_CHUNK,),
            in_specs=[spec(k) for k in range(len(orders)) for _ in range(4)],
            out_specs=pl.BlockSpec((None, None, 512, shape[-1]), lambda s, m: (s // 4, s % 4, 0, 0)),
        ),
        out_shape=jax.ShapeDtypeStruct(shape, jnp.bfloat16),
        compiler_params=pltpu.CompilerParams(dimension_semantics=("arbitrary",)),
        cost_estimate=pl.CostEstimate(flops=32 << 20, bytes_accessed=32 << 20, transcendentals=0),
        name="join_d_in",
    )(me, *[s for chunk in chunks for s in chunk])


def solution(mesh):
    dp_size, tp_size = mesh.shape["dp"], mesh.shape["tp"]
    CORE, X, Y = 1, 2, 4

    def swap(value, mask):
        return lax.ppermute(value, "tp", [(i, i ^ mask) for i in range(tp_size)])

    def add(a, b):
        return (a.astype(jnp.float32) + b.astype(jnp.float32)).astype(jnp.bfloat16)

    def sum_over_tp(keep, send, cot_piece, x_first):
        one, two = (X, Y) if x_first else (Y, X)
        got = swap(send, CORE)
        away, kept = add(keep[1], got[1]), add(keep[0], got[0])
        got = swap(away, one)
        away = add(kept[1], got[1])
        last = swap(away, two)
        mine = add(kept[0], got[0]).astype(jnp.float32) + last.astype(jnp.float32)
        piece = (cot_piece.astype(jnp.float32) + mine).astype(jnp.bfloat16)
        other = swap(piece, two)
        own = jnp.stack([piece, other])
        first = swap(own, one)
        core_own = swap(own, CORE)
        core_first = swap(first, CORE)
        return piece, (own, first, core_own, core_first)

    def local_pass(x_in, u_pre, w_up, w_down, d_out, noise_up, noise_down, clip_norm, noise_mult):
        n_layers = x_in.shape[0]
        micro, per_micro = d_out.shape[:2]
        examples = micro * per_micro * dp_size
        me = lax.axis_index("tp").astype(jnp.int32)
        my_dp = lax.axis_index("dp").astype(jnp.int32)
        me_arr = me.reshape(1)
        chunks = [(m, e) for m in range(micro) for e in range(0, per_micro, PER_CHUNK)]
        orders = [k % 2 == 0 for k in range(len(chunks))]
        cots = [d_out] * len(chunks)
        pieces = [None] * len(chunks)
        norms = [None] * len(chunks)
        saved = [None] * n_layers
        for layer in reversed(range(n_layers)):
            top = layer == n_layers - 1
            hids, dhids, full = [], [], []
            for k, (m, e) in enumerate(chunks):
                hidden, d_hid, keep, send, norms[k], cot = backward_chunk(
                    layer, m, e, orders[k], me_arr, cots[k], norms[k], x_in, u_pre, w_up, w_down
                )
                pieces[k], cots[k] = sum_over_tp(keep, send, cot if top else pieces[k], orders[k])
                hids.append(hidden)
                dhids.append(d_hid)
                full.append(cot)
            saved[layer] = (tuple(hids), tuple(dhids), d_out if top else tuple(full))
        d_in = join_slots(me_arr, orders, cots, d_out.shape)
        norm_vec = lax.psum(jnp.sum(jnp.concatenate(norms), axis=(1, 2)), "tp")
        clip = jnp.minimum(1.0, clip_norm[0] / jnp.sqrt(norm_vec))
        noise_scale = (noise_mult[0] * clip_norm[0]).reshape(1)
        own_half, other_half = my_dp.reshape(1), (1 - my_dp).reshape(1)
        swap_dp = [(i, 1 - i) for i in range(dp_size)]
        grads = [(up, layer) for layer in reversed(range(n_layers)) for up in (True, False)]

        def grad(up, layer, *rest):
            hids, dhids, full = saved[layer]
            lhs, rhs = (x_in, dhids) if up else (hids, full)
            return weight_grad(up, layer, rest[0], clip, lhs, rhs, *rest[1:])

        got = []
        for up, layer in grads:
            part = grad(up, layer, other_half)
            got.append(lax.ppermute(part, "dp", swap_dp))
        result = [None, None]
        for i, (up, layer) in enumerate(grads):
            own = grad(up, layer, own_half, noise_up if up else noise_down, noise_scale)
            if i == len(grads) - 1:
                own, d_in = lax.optimization_barrier((own, d_in))
            result[up] = finish_grad(layer, n_layers, examples, own, got[i], result[up])
        return result[1], result[0], d_in

    in_specs = (P(None, None, "dp", None, None), P(None, None, "dp", None, "tp"), P(None, None, "tp"), P(None, "tp", None), P(None, "dp", None, None), P(None, "dp", "tp"), P(None, "tp", "dp"), P(), P())
    out_specs = (P(None, "dp", "tp"), P(None, "tp", "dp"), P(None, "dp", None, None))
    return jax.shard_map(local_pass, mesh=mesh, in_specs=in_specs, out_specs=out_specs, check_vma=False)
```

```python
import functools
import math

import jax
import jax.numpy as jnp
from jax import lax
from jax.experimental import pallas as pl
from jax.experimental.pallas import tpu as pltpu
from jax.sharding import PartitionSpec as P


PIECE = 256
HALF = 1024
PER_CHUNK = 2
TANH_SCALE = math.sqrt(2.0 / math.pi)
TANH_CUBE = 0.044715

NT = (((1,), (1,)), ((), ()))
TN = (((0,), (0,)), ((), ()))


def dot(lhs, rhs, dims):
    return lax.dot_general(lhs, rhs, dims, preferred_element_type=jnp.float32)


def piece_of(me, r1, r2, rc, x_first):
    bits = (r2 * 4 + r1 * 2 + rc) if x_first else (r1 * 4 + r2 * 2 + rc)
    return me ^ bits


def hidden_of(u_ref, cot, w2, h_ref, dh_ref, before=lambda j: None):
    width = 256
    for j in range(u_ref.shape[-1] // width):
        before(j)
        cols = slice(j * width, (j + 1) * width)
        d_act = dot(cot[...], w2[cols, :], NT)
        u = u_ref[:, cols].astype(jnp.float32)
        u_sq = u * u
        t = jnp.tanh(TANH_SCALE * (u + TANH_CUBE * (u_sq * u)))
        cdf = 0.5 * (1.0 + t)
        slope = cdf + (0.5 * TANH_SCALE) * (1.0 - t * t) * (u * (1.0 + (3.0 * TANH_CUBE) * u_sq))
        h_ref[:, cols] = (u * cdf).astype(jnp.bfloat16)
        dh_ref[:, cols] = (slope * d_act).astype(jnp.bfloat16)


def backward_kernel(layer, micro, first_ex, x_first, from_slots, me_ref, *refs):
    *refs, w1, w2, x_buf, w1_sem, w2_sem, x_sem = refs
    if from_slots:
        own, first, core_own, core_first, norm_in, u_ref, w1_hbm, w2_hbm, x_hbm = refs[:9]
        h_ref, dh_ref, keep_ref, send_ref, norm_ref, dz_ref = refs[9:]
    else:
        dz_in, u_ref, w1_hbm, w2_hbm, x_hbm, h_ref, dh_ref, keep_ref, send_ref, norm_ref, piece_ref = refs
    me = me_ref[0]
    step = pl.program_id(0)
    slots = [(rc, r1, r2) for rc in (1, 0) for r1 in range(2) for r2 in range(2)]
    hid = u_ref.shape[-1]

    def rows_of(rc, r1, r2):
        return pl.ds(pl.multiple_of(piece_of(me, r1, r2, rc, x_first) * PIECE, PIECE), PIECE)

    def w2_copy(i):
        rows = pl.ds(i * (hid // 2), hid // 2)
        return pltpu.make_async_copy(w2_hbm.at[layer, rows, :], w2.at[rows, :], w2_sem.at[i])

    def w1_copy(i):
        return pltpu.make_async_copy(w1_hbm.at[layer, rows_of(*slots[i]), :], w1.at[i], w1_sem.at[i])

    def x_copy():
        return pltpu.make_async_copy(x_hbm.at[layer, micro, first_ex + step], x_buf, x_sem)

    @pl.when(step == 0)
    def _():
        for i in range(2):
            w2_copy(i).start()
        for i in range(8):
            w1_copy(i).start()

    x_copy().start()
    if from_slots:
        for rc, r1, slot in ((0, 0, own), (0, 1, first), (1, 0, core_own), (1, 1, core_first)):
            for r2 in range(2):
                dz_ref[:, rows_of(rc, r1, r2)] = slot[r2]
        cot = dz_ref
    else:
        cot = dz_in
        piece_ref[...] = dz_in[:, pl.ds(pl.multiple_of(me * PIECE, PIECE), PIECE)]

    def wait_weights(j):
        if j % 2 == 0:

            @pl.when(step == 0)
            def _():
                w2_copy(j // 2).wait()

    hidden_of(u_ref, cot, w2, h_ref, dh_ref, wait_weights)

    @pl.when(step == 0)
    def _():
        for i in range(8):
            w1_copy(i).wait()

    for i, (rc, r1, r2) in enumerate(slots):
        out = send_ref if rc else keep_ref
        out[r1, r2] = dot(dh_ref[...], w1[i], NT).astype(jnp.bfloat16)

    def gram_product(left, right):
        prod = dot(left[...], left[:256, :], NT) * dot(right[...], right[:256, :], NT)
        corner = dot(left[256:, :], left[256:, :], NT) * dot(right[256:, :], right[256:, :], NT)
        total = prod[:256] + 2.0 * prod[256:] + corner
        return jnp.sum(total.reshape(32, 8, 256), axis=0)

    norm = gram_product(h_ref, cot)
    x_copy().wait()
    norm += gram_product(dh_ref, x_buf)
    norm_ref[...] = norm_in[...] + norm if from_slots else norm


def backward_chunk(layer, micro, first_ex, x_first, me, dz_inputs, norm_in, x_in, u_pre, w_up, w_down):
    rows = PER_CHUNK * 512
    hid, model = u_pre.shape[-1], w_up.shape[1]
    from_slots = isinstance(dz_inputs, tuple)
    norm_spec = pl.BlockSpec((None, 8, 256), lambda e, m: (e, 0, 0))
    piece_spec = pl.BlockSpec((512, PIECE), lambda e, m: (e, 0))
    if from_slots:
        in_specs = [pl.BlockSpec((2, 512, PIECE), lambda e, m: (0, e, 0))] * 4 + [norm_spec]
        operands = (*dz_inputs, norm_in)
    else:
        in_specs = [pl.BlockSpec((None, None, 512, model), lambda e, m: (micro, first_ex + e, 0, 0))]
        operands = (dz_inputs,)
    part_spec = pl.BlockSpec((2, 2, 512, PIECE), lambda e, m: (0, 0, e, 0))
    part_shape = jax.ShapeDtypeStruct((2, 2, rows, PIECE), jnp.bfloat16)
    act_spec = pl.BlockSpec((512, hid), lambda e, m: (e, 0))
    act_shape = jax.ShapeDtypeStruct((rows, hid), jnp.bfloat16)
    last_cols = model if from_slots else PIECE
    any_spec = pl.BlockSpec(memory_space=pl.ANY)
    return pl.pallas_call(
        functools.partial(backward_kernel, layer, micro, first_ex, x_first, from_slots),
        grid_spec=pltpu.PrefetchScalarGridSpec(
            num_scalar_prefetch=1,
            grid=(PER_CHUNK,),
            in_specs=in_specs
            + [pl.BlockSpec((None, None, None, 512, hid), lambda e, m: (layer, micro, first_ex + e, 0, 0))]
            + [any_spec] * 3,
            out_specs=[act_spec, act_spec, part_spec, part_spec, norm_spec]
            + [pl.BlockSpec((512, last_cols), lambda e, m: (e, 0))],
            scratch_shapes=[
                pltpu.VMEM((8, PIECE, hid), jnp.bfloat16),
                pltpu.VMEM((hid, model), jnp.bfloat16),
                pltpu.VMEM((512, model), jnp.bfloat16),
                pltpu.SemaphoreType.DMA((8,)),
                pltpu.SemaphoreType.DMA((2,)),
                pltpu.SemaphoreType.DMA,
            ],
        ),
        out_shape=[act_shape, act_shape, part_shape, part_shape]
        + [jax.ShapeDtypeStruct((PER_CHUNK, 8, 256), jnp.float32), jax.ShapeDtypeStruct((rows, last_cols), jnp.bfloat16)],
        compiler_params=pltpu.CompilerParams(dimension_semantics=("arbitrary",)),
        cost_estimate=pl.CostEstimate(flops=6 * rows * hid * model, bytes_accessed=24 << 20, transcendentals=rows * hid),
    )(me, *operands, u_pre, w_up, w_down, x_in)


def grad_kernel(sizes, half_ref, clip_ref, *refs):
    n_lhs, n_rhs, per, has_init = sizes
    if has_init:
        scale_ref, init_ref, *refs = refs
    lhs, rhs, out_ref = refs[:n_lhs], refs[n_lhs:-1], refs[-1]
    step = pl.program_id(0)

    @pl.when(step == 0)
    def _():
        out_ref[...] = scale_ref[0] * init_ref[...] if has_init else jnp.zeros_like(out_ref)

    clip = clip_ref[step]
    for k in range(max(n_lhs, n_rhs)):

        @pl.when(step // per == k)
        def _(k=k):
            a = lhs[min(k, n_lhs - 1)]
            b = rhs[min(k, n_rhs - 1)]
            scaled = (b[...].astype(jnp.float32) * clip).astype(jnp.bfloat16)
            for j in range(2):
                cols = slice(j * 512, (j + 1) * 512)
                out_ref[:, cols] += dot(a[...], scaled[:, cols], TN)


def grad_operand(value, layer, per, columns):
    def col(h):
        return 0 if columns is None else h[0]

    if isinstance(value, tuple):
        return value, [
            pl.BlockSpec((512, 1024), lambda s, h, k=k: (jnp.clip(s - per * k, 0, per - 1), col(h))) for k in range(len(value))
        ]
    lead = {5: lambda s: (layer, s // 4, s % 4), 4: lambda s: (s // 4, s % 4), 3: lambda s: (s,)}[value.ndim]
    return (value,), [pl.BlockSpec((None,) * (value.ndim - 2) + (512, 1024), lambda s, h: (*lead(s), 0, col(h)))]


def weight_grad(layer, half, clip, lhs, rhs, lhs_half, rhs_half, init=None, init_layer=0, scale=None):
    parts = max(len(v) if isinstance(v, tuple) else 1 for v in (lhs, rhs))
    n_ex = clip.shape[0]
    per = n_ex // parts
    lhs, lhs_specs = grad_operand(lhs, layer, per, lhs_half)
    rhs, rhs_specs = grad_operand(rhs, layer, per, rhs_half)
    lead, lead_specs = (), []
    if init is not None:
        lead = (scale, init)
        lead_specs = [pl.BlockSpec(memory_space=pltpu.SMEM), pl.BlockSpec((None, 1024, 1024), lambda s, h: (init_layer, 0, 0))]
    return pl.pallas_call(
        functools.partial(grad_kernel, (len(lhs), len(rhs), per, init is not None)),
        grid_spec=pltpu.PrefetchScalarGridSpec(
            num_scalar_prefetch=1,
            grid=(n_ex,),
            in_specs=[pl.BlockSpec(memory_space=pltpu.SMEM)] + lead_specs + lhs_specs + rhs_specs,
            out_specs=pl.BlockSpec((1024, 1024), lambda s, h: (0, 0)),
        ),
        out_shape=jax.ShapeDtypeStruct((1024, 1024), jnp.float32),
        compiler_params=pltpu.CompilerParams(dimension_semantics=("arbitrary",)),
        cost_estimate=pl.CostEstimate(flops=2 * n_ex * 512 * 1024 * 1024, bytes_accessed=24 << 20, transcendentals=0),
    )(half, clip, *lead, *lhs, *rhs)


def hidden_kernel(u_ref, dz_ref, w2_ref, h_ref, dh_ref):
    hidden_of(u_ref, dz_ref, w2_ref, h_ref, dh_ref)


def hidden_again(layer, u_other, cot_other, w_down):
    n_ex, _, model = cot_other.shape
    hid = u_other.shape[-1]
    act_spec = pl.BlockSpec((512, hid), lambda e: (e, 0))
    act_shape = jax.ShapeDtypeStruct((n_ex * 512, hid), jnp.bfloat16)
    return pl.pallas_call(
        hidden_kernel,
        grid=(n_ex,),
        in_specs=[
            pl.BlockSpec((None, 512, hid), lambda e: (e, 0, 0)),
            pl.BlockSpec((None, 512, model), lambda e: (e, 0, 0)),
            pl.BlockSpec((None, hid, model), lambda e: (layer, 0, 0)),
        ],
        out_specs=[act_spec, act_spec],
        out_shape=[act_shape, act_shape],
        compiler_params=pltpu.CompilerParams(dimension_semantics=("arbitrary",)),
        cost_estimate=pl.CostEstimate(flops=2 * n_ex * 512 * hid * model, bytes_accessed=48 << 20, transcendentals=n_ex * 512 * hid),
        name="hidden_again",
    )(u_other, cot_other, w_down)


def finish_kernel(inv, has_got, own_ref, *refs):
    total = own_ref[...] + refs[0][...] if has_got else own_ref[...]
    refs[-1][...] = total * inv


def finish_grad(layer, n_layers, examples, own, got, buffer):
    spec = pl.BlockSpec((256, 1024), lambda i: (i, 0))
    operands = (own,) if got is None else (own, got)
    in_specs, aliases = [spec] * len(operands), {}
    if buffer is not None:
        aliases = {len(operands): 0}
        operands += (buffer,)
        in_specs.append(pl.BlockSpec(memory_space=pl.ANY))
    return pl.pallas_call(
        functools.partial(finish_kernel, 1.0 / examples, got is not None),
        grid=(4,),
        in_specs=in_specs,
        out_specs=pl.BlockSpec((None, 256, 1024), lambda i: (layer, i, 0)),
        out_shape=jax.ShapeDtypeStruct((n_layers, 1024, 1024), jnp.float32),
        input_output_aliases=aliases,
        compiler_params=pltpu.CompilerParams(dimension_semantics=("arbitrary",)),
        cost_estimate=pl.CostEstimate(flops=12 << 20, bytes_accessed=12 << 20, transcendentals=0),
    )(*operands)


def join_kernel(orders, me_ref, *refs):
    out_ref = refs[-1]
    step = pl.program_id(0)
    for k, x_first in enumerate(orders):

        @pl.when(step // PER_CHUNK == k)
        def _(k=k, x_first=x_first):
            own, first, core_own, core_first = refs[4 * k : 4 * k + 4]
            for rc, r1, slots in ((0, 0, own), (0, 1, first), (1, 0, core_own), (1, 1, core_first)):
                for r2 in range(2):
                    start = pl.multiple_of(piece_of(me_ref[0], r1, r2, rc, x_first) * PIECE, PIECE)
                    out_ref[:, pl.ds(start, PIECE)] = slots[r2]


def join_slots(me, orders, chunks, shape):
    def spec(k):
        return pl.BlockSpec((2, 512, PIECE), lambda s, m: (0, jnp.clip(s - PER_CHUNK * k, 0, PER_CHUNK - 1), 0))

    return pl.pallas_call(
        functools.partial(join_kernel, orders),
        grid_spec=pltpu.PrefetchScalarGridSpec(
            num_scalar_prefetch=1,
            grid=(len(orders) * PER_CHUNK,),
            in_specs=[spec(k) for k in range(len(orders)) for _ in range(4)],
            out_specs=pl.BlockSpec((None, None, 512, shape[-1]), lambda s, m: (s // 4, s % 4, 0, 0)),
        ),
        out_shape=jax.ShapeDtypeStruct(shape, jnp.bfloat16),
        compiler_params=pltpu.CompilerParams(dimension_semantics=("arbitrary",)),
        cost_estimate=pl.CostEstimate(flops=32 << 20, bytes_accessed=32 << 20, transcendentals=0),
        name="join_d_in",
    )(me, *[s for chunk in chunks for s in chunk])


def solution(mesh):
    dp_size, tp_size = mesh.shape["dp"], mesh.shape["tp"]
    CORE, X, Y = 1, 2, 4

    def swap(value, mask):
        return lax.ppermute(value, "tp", [(i, i ^ mask) for i in range(tp_size)])

    def add(a, b):
        return (a.astype(jnp.float32) + b.astype(jnp.float32)).astype(jnp.bfloat16)

    def sum_over_tp(keep, send, cot_piece, x_first):
        one, two = (X, Y) if x_first else (Y, X)
        got = swap(send, CORE)
        away, kept = add(keep[1], got[1]), add(keep[0], got[0])
        got = swap(away, one)
        away = add(kept[1], got[1])
        last = swap(away, two)
        mine = add(kept[0], got[0]).astype(jnp.float32) + last.astype(jnp.float32)
        piece = (cot_piece.astype(jnp.float32) + mine).astype(jnp.bfloat16)
        other = swap(piece, two)
        own = jnp.stack([piece, other])
        first = swap(own, one)
        core_own = swap(own, CORE)
        core_first = swap(first, CORE)
        return piece, (own, first, core_own, core_first)

    def local_pass(x_in, u_pre, w_up, w_down, d_out, noise_up, noise_down, clip_norm, noise_mult):
        n_layers = x_in.shape[0]
        micro, per_micro = d_out.shape[:2]
        examples = micro * per_micro * dp_size
        me = lax.axis_index("tp").astype(jnp.int32)
        my_dp = lax.axis_index("dp").astype(jnp.int32)
        me_arr = me.reshape(1)
        chunks = [(m, e) for m in range(micro) for e in range(0, per_micro, PER_CHUNK)]
        orders = [k % 2 == 0 for k in range(len(chunks))]
        cots = [d_out] * len(chunks)
        pieces = [None] * len(chunks)
        norms = [None] * len(chunks)
        saved = [None] * n_layers
        top = n_layers - 1
        swap_dp = [(i, 1 - i) for i in range(dp_size)]
        ex_all = micro * per_micro
        cot_slice = lax.dynamic_index_in_dim(d_out.reshape(ex_all, *d_out.shape[2:]), me, 0)
        x_slice = lax.dynamic_slice(
            x_in[top].reshape(ex_all, *d_out.shape[2:]), (me, 0, (1 - my_dp) * HALF), (1, d_out.shape[2], HALF)
        )
        cot_other = lax.ppermute(cot_slice, "dp", swap_dp)
        u_other = lax.ppermute(u_pre[top].reshape(ex_all, *u_pre.shape[3:]), "dp", swap_dp)
        x_other = lax.ppermute(x_slice, "dp", swap_dp)
        for layer in reversed(range(n_layers)):
            top = layer == n_layers - 1
            hids, dhids, full = [], [], []
            for k, (m, e) in enumerate(chunks):
                hidden, d_hid, keep, send, norms[k], cot = backward_chunk(
                    layer, m, e, orders[k], me_arr, cots[k], norms[k], x_in, u_pre, w_up, w_down
                )
                if (layer, k) == (0, 1):
                    cot_other, x_other, norms[k] = lax.optimization_barrier((cot_other, x_other, norms[k]))
                pieces[k], cots[k] = sum_over_tp(keep, send, cot if top else pieces[k], orders[k])
                hids.append(hidden)
                dhids.append(d_hid)
                full.append(cot)
            saved[layer] = (tuple(hids), tuple(dhids), d_out if top else tuple(full))
        cot_other = lax.all_gather(cot_other, "tp", axis=0, tiled=True)
        x_other = lax.all_gather(x_other, "tp", axis=0, tiled=True)
        hid_other, dhid_other = hidden_again(n_layers - 1, u_other, cot_other, w_down)
        d_in = join_slots(me_arr, orders, cots, d_out.shape)
        norm_vec = lax.psum(jnp.sum(jnp.concatenate(norms), axis=(1, 2)), "tp")
        clip = jnp.minimum(1.0, clip_norm[0] / jnp.sqrt(norm_vec))
        noise_scale = (noise_mult[0] * clip_norm[0]).reshape(1)
        own_half, other_half = my_dp.reshape(1), (1 - my_dp).reshape(1)
        top = n_layers - 1
        grads = [(up, layer) for layer in reversed(range(top)) for up in (True, False)]

        def grad(up, layer, half, *init):
            hids, dhids, full = saved[layer]
            lhs, rhs = (x_in, dhids) if up else (hids, full)
            return weight_grad(layer, half, clip, lhs, rhs, True if up else None, None if up else True, *init)

        got = []
        for up, layer in grads:
            part = grad(up, layer, other_half)
            got.append(lax.ppermute(part, "dp", swap_dp))
        result = [None, None]
        clip_other = lax.ppermute(clip, "dp", swap_dp)
        one = jnp.ones((1,), jnp.float32)
        for up in (True, False):
            own = grad(up, top, own_half, noise_up if up else noise_down, top, noise_scale)[None]
            lhs, rhs = (x_other, (dhid_other,)) if up else ((hid_other,), cot_other)
            own = weight_grad(top, own_half, clip_other, lhs, rhs, None, None if up else True, own, 0, one)
            result[up] = finish_grad(top, n_layers, examples, own, None, None)
        for i, (up, layer) in enumerate(grads):
            own = grad(up, layer, own_half, noise_up if up else noise_down, layer, noise_scale)
            if i == len(grads) - 1:
                own, d_in = lax.optimization_barrier((own, d_in))
            result[up] = finish_grad(layer, n_layers, examples, own, got[i], result[up])
        return result[1], result[0], d_in

    in_specs = (P(None, None, "dp", None, None), P(None, None, "dp", None, "tp"), P(None, None, "tp"), P(None, "tp", None), P(None, "dp", None, None), P(None, "dp", "tp"), P(None, "tp", "dp"), P(), P())
    out_specs = (P(None, "dp", "tp"), P(None, "tp", "dp"), P(None, "dp", None, None))
    return jax.shard_map(local_pass, mesh=mesh, in_specs=in_specs, out_specs=out_specs, check_vma=False)
```

```python
import functools
import math

import jax
import jax.numpy as jnp
from jax import lax
from jax.experimental import pallas as pl
from jax.experimental.pallas import tpu as pltpu
from jax.sharding import PartitionSpec as P


PIECE = 256
HALF = 1024
PER_CHUNK = 2
TANH_SCALE = math.sqrt(2.0 / math.pi)
TANH_CUBE = 0.044715

NT = (((1,), (1,)), ((), ()))
TN = (((0,), (0,)), ((), ()))


def dot(lhs, rhs, dims):
    return lax.dot_general(lhs, rhs, dims, preferred_element_type=jnp.float32)


def piece_of(me, r1, r2, rc, x_first):
    bits = (r2 * 4 + r1 * 2 + rc) if x_first else (r1 * 4 + r2 * 2 + rc)
    return me ^ bits


def hidden_of(u_ref, cot, w2, h_ref, dh_ref, before=lambda j: None):
    width = 256
    for j in range(u_ref.shape[-1] // width):
        before(j)
        cols = slice(j * width, (j + 1) * width)
        d_act = dot(cot[...], w2[cols, :], NT)
        u = u_ref[:, cols].astype(jnp.float32)
        u_sq = u * u
        t = jnp.tanh(TANH_SCALE * (u + TANH_CUBE * (u_sq * u)))
        cdf = 0.5 * (1.0 + t)
        slope = cdf + (0.5 * TANH_SCALE) * (1.0 - t * t) * (u * (1.0 + (3.0 * TANH_CUBE) * u_sq))
        h_ref[:, cols] = (u * cdf).astype(jnp.bfloat16)
        dh_ref[:, cols] = (slope * d_act).astype(jnp.bfloat16)


def backward_kernel(layer, micro, first_ex, x_first, from_slots, me_ref, *refs):
    *refs, w1, w2, x_buf, w1_sem, w2_sem, x_sem = refs
    if from_slots:
        own, first, core_own, core_first, norm_in, u_ref, w1_hbm, w2_hbm, x_hbm = refs[:9]
        h_ref, dh_ref, keep_ref, send_ref, norm_ref, dz_ref = refs[9:]
    else:
        dz_in, u_ref, w1_hbm, w2_hbm, x_hbm, h_ref, dh_ref, keep_ref, send_ref, norm_ref, piece_ref = refs
    me = me_ref[0]
    step = pl.program_id(0)
    slots = [(rc, r1, r2) for rc in (1, 0) for r1 in range(2) for r2 in range(2)]
    hid = u_ref.shape[-1]

    def rows_of(rc, r1, r2):
        return pl.ds(pl.multiple_of(piece_of(me, r1, r2, rc, x_first) * PIECE, PIECE), PIECE)

    def w2_copy(i):
        rows = pl.ds(i * (hid // 2), hid // 2)
        return pltpu.make_async_copy(w2_hbm.at[layer, rows, :], w2.at[rows, :], w2_sem.at[i])

    def w1_copy(i):
        return pltpu.make_async_copy(w1_hbm.at[layer, rows_of(*slots[i]), :], w1.at[i], w1_sem.at[i])

    def x_copy():
        return pltpu.make_async_copy(x_hbm.at[layer, micro, first_ex + step], x_buf, x_sem)

    @pl.when(step == 0)
    def _():
        for i in range(2):
            w2_copy(i).start()
        for i in range(8):
            w1_copy(i).start()

    x_copy().start()
    if from_slots:
        for rc, r1, slot in ((0, 0, own), (0, 1, first), (1, 0, core_own), (1, 1, core_first)):
            for r2 in range(2):
                dz_ref[:, rows_of(rc, r1, r2)] = slot[r2]
        cot = dz_ref
    else:
        cot = dz_in
        piece_ref[...] = dz_in[:, pl.ds(pl.multiple_of(me * PIECE, PIECE), PIECE)]

    def wait_weights(j):
        if j % 2 == 0:

            @pl.when(step == 0)
            def _():
                w2_copy(j // 2).wait()

    hidden_of(u_ref, cot, w2, h_ref, dh_ref, wait_weights)

    @pl.when(step == 0)
    def _():
        for i in range(8):
            w1_copy(i).wait()

    for i, (rc, r1, r2) in enumerate(slots):
        out = send_ref if rc else keep_ref
        out[r1, r2] = dot(dh_ref[...], w1[i], NT).astype(jnp.bfloat16)

    def gram_product(left, right):
        prod = dot(left[...], left[:256, :], NT) * dot(right[...], right[:256, :], NT)
        corner = dot(left[256:, :], left[256:, :], NT) * dot(right[256:, :], right[256:, :], NT)
        total = prod[:256] + 2.0 * prod[256:] + corner
        return jnp.sum(total.reshape(32, 8, 256), axis=0)

    norm = gram_product(h_ref, cot)
    x_copy().wait()
    norm += gram_product(dh_ref, x_buf)
    norm_ref[...] = norm_in[...] + norm if from_slots else norm


def backward_chunk(layer, micro, first_ex, x_first, me, dz_inputs, norm_in, x_in, u_pre, w_up, w_down):
    rows = PER_CHUNK * 512
    hid, model = u_pre.shape[-1], w_up.shape[1]
    from_slots = isinstance(dz_inputs, tuple)
    norm_spec = pl.BlockSpec((None, 8, 256), lambda e, m: (e, 0, 0))
    piece_spec = pl.BlockSpec((512, PIECE), lambda e, m: (e, 0))
    if from_slots:
        in_specs = [pl.BlockSpec((2, 512, PIECE), lambda e, m: (0, e, 0))] * 4 + [norm_spec]
        operands = (*dz_inputs, norm_in)
    else:
        in_specs = [pl.BlockSpec((None, None, 512, model), lambda e, m: (micro, first_ex + e, 0, 0))]
        operands = (dz_inputs,)
    part_spec = pl.BlockSpec((2, 2, 512, PIECE), lambda e, m: (0, 0, e, 0))
    part_shape = jax.ShapeDtypeStruct((2, 2, rows, PIECE), jnp.bfloat16)
    act_spec = pl.BlockSpec((512, hid), lambda e, m: (e, 0))
    act_shape = jax.ShapeDtypeStruct((rows, hid), jnp.bfloat16)
    last_cols = model if from_slots else PIECE
    any_spec = pl.BlockSpec(memory_space=pl.ANY)
    return pl.pallas_call(
        functools.partial(backward_kernel, layer, micro, first_ex, x_first, from_slots),
        grid_spec=pltpu.PrefetchScalarGridSpec(
            num_scalar_prefetch=1,
            grid=(PER_CHUNK,),
            in_specs=in_specs
            + [pl.BlockSpec((None, None, None, 512, hid), lambda e, m: (layer, micro, first_ex + e, 0, 0))]
            + [any_spec] * 3,
            out_specs=[act_spec, act_spec, part_spec, part_spec, norm_spec]
            + [pl.BlockSpec((512, last_cols), lambda e, m: (e, 0))],
            scratch_shapes=[
                pltpu.VMEM((8, PIECE, hid), jnp.bfloat16),
                pltpu.VMEM((hid, model), jnp.bfloat16),
                pltpu.VMEM((512, model), jnp.bfloat16),
                pltpu.SemaphoreType.DMA((8,)),
                pltpu.SemaphoreType.DMA((2,)),
                pltpu.SemaphoreType.DMA,
            ],
        ),
        out_shape=[act_shape, act_shape, part_shape, part_shape]
        + [jax.ShapeDtypeStruct((PER_CHUNK, 8, 256), jnp.float32), jax.ShapeDtypeStruct((rows, last_cols), jnp.bfloat16)],
        compiler_params=pltpu.CompilerParams(dimension_semantics=("arbitrary",)),
        cost_estimate=pl.CostEstimate(flops=6 * rows * hid * model, bytes_accessed=24 << 20, transcendentals=rows * hid),
    )(me, *operands, u_pre, w_up, w_down, x_in)


def grad_kernel(segs, n_lhs, n_rhs, init_layer, has_init, has_got, inv, half_ref, clip_ref, *refs):
    refs = list(refs)
    scale_ref = refs.pop(0) if has_init else None
    lhs = [refs.pop(0) for _ in range(n_lhs)]
    rhs = [refs.pop(0) for _ in range(n_rhs)]
    init = refs.pop(0) if has_init else None
    got = refs.pop(0) if has_got else None
    out_ref, a_buf, b_buf, a_sem, b_sem, *extra = refs[-5 - 2 * (has_init + has_got) :]
    init_buf, init_sem = extra[:2] if has_init else (None, None)
    got_buf, got_sem = extra[-2:] if has_got else (None, None)
    half = half_ref[0]
    step = pl.program_id(0)
    n_steps = pl.num_programs(0)

    def view(ref, kind, e):
        layer, cols = kind
        cols = pl.ds(pl.multiple_of(half * HALF, HALF), HALF) if cols else pl.ds(0, 1024)
        if layer is not None:
            return ref.at[layer, e // 4, e % 4, :, cols]
        if len(ref.shape) == 4:
            return ref.at[e // 4, e % 4, :, cols]
        if len(ref.shape) == 3:
            return ref.at[e, :, cols]
        return ref.at[pl.ds(pl.multiple_of(e * 512, 512), 512), cols]

    def fetch(at, slot):
        for start, count, left, left_kind, left_first, right, right_kind, right_first in segs:

            @pl.when(jnp.logical_and(at >= start, at < start + count))
            def _():
                e = at - start
                pltpu.make_async_copy(view(lhs[left], left_kind, e + left_first), a_buf.at[slot], a_sem.at[slot]).start()
                pltpu.make_async_copy(view(rhs[right], right_kind, e + right_first), b_buf.at[slot], b_sem.at[slot]).start()

    slot = step % 2

    @pl.when(step == 0)
    def _():
        fetch(0, 0)
        out_ref[...] = jnp.zeros_like(out_ref)

    @pl.when(step + 1 < n_steps)
    def _():
        fetch(step + 1, 1 - slot)

    @pl.when(step == 1)
    def _():
        if has_init:
            pltpu.make_async_copy(init.at[init_layer], init_buf, init_sem).start()
        if has_got:
            pltpu.make_async_copy(got, got_buf, got_sem).start()

    pltpu.make_async_copy(a_buf.at[slot], a_buf.at[slot], a_sem.at[slot]).wait()
    pltpu.make_async_copy(b_buf.at[slot], b_buf.at[slot], b_sem.at[slot]).wait()
    scaled = (b_buf[slot].astype(jnp.float32) * clip_ref[step]).astype(jnp.bfloat16)
    for j in range(2):
        cols = slice(j * 512, (j + 1) * 512)
        out_ref[:, cols] += dot(a_buf[slot], scaled[:, cols], TN)

    if has_init or has_got:

        @pl.when(step == n_steps - 1)
        def _():
            total = out_ref[...]
            if has_init:
                pltpu.make_async_copy(init.at[init_layer], init_buf, init_sem).wait()
                total = total + scale_ref[0] * init_buf[...]
            if has_got:
                pltpu.make_async_copy(got, got_buf, got_sem).wait()
                total = total + got_buf[...]
            out_ref[...] = total * inv if inv is not None else total


def weight_grad(half, clip, segs, init=None, got=None, inv=None, result=None):
    lhs, rhs, table, at = [], [], [], 0

    def place(group, value):
        for i, other in enumerate(group):
            if other is value:
                return i
        group.append(value)
        return len(group) - 1

    for count, (a, a_layer, a_half, a_first), (b, b_layer, b_half, b_first) in segs:
        left, right = place(lhs, a), place(rhs, b)
        table.append((at, count, left, (a_layer, a_half), a_first, right, (b_layer, b_half), b_first))
        at += count
    any_spec = pl.BlockSpec(memory_space=pl.ANY)
    smem_spec = pl.BlockSpec(memory_space=pltpu.SMEM)
    operands, in_specs = [clip], [smem_spec]
    scratch = [
        pltpu.VMEM((2, 512, 1024), jnp.bfloat16),
        pltpu.VMEM((2, 512, 1024), jnp.bfloat16),
        pltpu.SemaphoreType.DMA((2,)),
        pltpu.SemaphoreType.DMA((2,)),
    ]
    if init is not None:
        operands.append(init[2])
        in_specs.append(smem_spec)
    operands += lhs + rhs
    in_specs += [any_spec] * (len(lhs) + len(rhs))
    for value in (init[0] if init is not None else None, got):
        if value is not None:
            operands.append(value)
            in_specs.append(any_spec)
            scratch += [pltpu.VMEM((1024, 1024), jnp.float32), pltpu.SemaphoreType.DMA]
    aliases = {}
    out_spec, out_shape = pl.BlockSpec((1024, 1024), lambda s, h: (0, 0)), (1024, 1024)
    if result is not None:
        out_layer, n_layers, buffer = result
        out_spec, out_shape = pl.BlockSpec((None, 1024, 1024), lambda s, h: (out_layer, 0, 0)), (n_layers, 1024, 1024)
        if buffer is not None:
            aliases = {len(operands) + 1: 0}
            operands.append(buffer)
            in_specs.append(any_spec)
    return pl.pallas_call(
        functools.partial(
            grad_kernel, table, len(lhs), len(rhs), init[1] if init is not None else 0, init is not None, got is not None, inv
        ),
        grid_spec=pltpu.PrefetchScalarGridSpec(
            num_scalar_prefetch=1, grid=(at,), in_specs=in_specs, out_specs=out_spec, scratch_shapes=scratch
        ),
        out_shape=jax.ShapeDtypeStruct(out_shape, jnp.float32),
        input_output_aliases=aliases,
        compiler_params=pltpu.CompilerParams(dimension_semantics=("arbitrary",)),
        cost_estimate=pl.CostEstimate(flops=2 * at * 512 * 1024 * 1024, bytes_accessed=24 << 20, transcendentals=0),
    )(half, *operands)


def hidden_kernel(u_ref, dz_ref, w2_ref, h_ref, dh_ref):
    hidden_of(u_ref, dz_ref, w2_ref, h_ref, dh_ref)


def hidden_again(layer, u_other, cot_other, w_down):
    n_ex, _, model = cot_other.shape
    hid = u_other.shape[-1]
    act_spec = pl.BlockSpec((512, hid), lambda e: (e, 0))
    act_shape = jax.ShapeDtypeStruct((n_ex * 512, hid), jnp.bfloat16)
    return pl.pallas_call(
        hidden_kernel,
        grid=(n_ex,),
        in_specs=[
            pl.BlockSpec((None, 512, hid), lambda e: (e, 0, 0)),
            pl.BlockSpec((None, 512, model), lambda e: (e, 0, 0)),
            pl.BlockSpec((None, hid, model), lambda e: (layer, 0, 0)),
        ],
        out_specs=[act_spec, act_spec],
        out_shape=[act_shape, act_shape],
        compiler_params=pltpu.CompilerParams(dimension_semantics=("arbitrary",)),
        cost_estimate=pl.CostEstimate(flops=2 * n_ex * 512 * hid * model, bytes_accessed=48 << 20, transcendentals=n_ex * 512 * hid),
        name="hidden_again",
    )(u_other, cot_other, w_down)


def finish_kernel(inv, has_got, own_ref, *refs):
    total = own_ref[...] + refs[0][...] if has_got else own_ref[...]
    refs[-1][...] = total * inv


def finish_grad(layer, n_layers, examples, own, got, buffer):
    spec = pl.BlockSpec((256, 1024), lambda i: (i, 0))
    operands = (own,) if got is None else (own, got)
    in_specs, aliases = [spec] * len(operands), {}
    if buffer is not None:
        aliases = {len(operands): 0}
        operands += (buffer,)
        in_specs.append(pl.BlockSpec(memory_space=pl.ANY))
    return pl.pallas_call(
        functools.partial(finish_kernel, 1.0 / examples, got is not None),
        grid=(4,),
        in_specs=in_specs,
        out_specs=pl.BlockSpec((None, 256, 1024), lambda i: (layer, i, 0)),
        out_shape=jax.ShapeDtypeStruct((n_layers, 1024, 1024), jnp.float32),
        input_output_aliases=aliases,
        compiler_params=pltpu.CompilerParams(dimension_semantics=("arbitrary",)),
        cost_estimate=pl.CostEstimate(flops=12 << 20, bytes_accessed=12 << 20, transcendentals=0),
    )(*operands)


def join_kernel(orders, me_ref, *refs):
    out_ref = refs[-1]
    step = pl.program_id(0)
    for k, x_first in enumerate(orders):

        @pl.when(step // PER_CHUNK == k)
        def _(k=k, x_first=x_first):
            own, first, core_own, core_first = refs[4 * k : 4 * k + 4]
            for rc, r1, slots in ((0, 0, own), (0, 1, first), (1, 0, core_own), (1, 1, core_first)):
                for r2 in range(2):
                    start = pl.multiple_of(piece_of(me_ref[0], r1, r2, rc, x_first) * PIECE, PIECE)
                    out_ref[:, pl.ds(start, PIECE)] = slots[r2]


def join_slots(me, orders, chunks, shape):
    def spec(k):
        return pl.BlockSpec((2, 512, PIECE), lambda s, m: (0, jnp.clip(s - PER_CHUNK * k, 0, PER_CHUNK - 1), 0))

    return pl.pallas_call(
        functools.partial(join_kernel, orders),
        grid_spec=pltpu.PrefetchScalarGridSpec(
            num_scalar_prefetch=1,
            grid=(len(orders) * PER_CHUNK,),
            in_specs=[spec(k) for k in range(len(orders)) for _ in range(4)],
            out_specs=pl.BlockSpec((None, None, 512, shape[-1]), lambda s, m: (s // 4, s % 4, 0, 0)),
        ),
        out_shape=jax.ShapeDtypeStruct(shape, jnp.bfloat16),
        compiler_params=pltpu.CompilerParams(dimension_semantics=("arbitrary",)),
        cost_estimate=pl.CostEstimate(flops=32 << 20, bytes_accessed=32 << 20, transcendentals=0),
        name="join_d_in",
    )(me, *[s for chunk in chunks for s in chunk])


def solution(mesh):
    dp_size, tp_size = mesh.shape["dp"], mesh.shape["tp"]
    CORE, X, Y = 1, 2, 4

    def swap(value, mask):
        return lax.ppermute(value, "tp", [(i, i ^ mask) for i in range(tp_size)])

    def add(a, b):
        return (a.astype(jnp.float32) + b.astype(jnp.float32)).astype(jnp.bfloat16)

    def sum_over_tp(keep, send, cot_piece, x_first):
        one, two = (X, Y) if x_first else (Y, X)
        got = swap(send, CORE)
        away, kept = add(keep[1], got[1]), add(keep[0], got[0])
        got = swap(away, one)
        away = add(kept[1], got[1])
        last = swap(away, two)
        mine = add(kept[0], got[0]).astype(jnp.float32) + last.astype(jnp.float32)
        piece = (cot_piece.astype(jnp.float32) + mine).astype(jnp.bfloat16)
        other = swap(piece, two)
        own = jnp.stack([piece, other])
        first = swap(own, one)
        core_own = swap(own, CORE)
        core_first = swap(first, CORE)
        return piece, (own, first, core_own, core_first)

    def local_pass(x_in, u_pre, w_up, w_down, d_out, noise_up, noise_down, clip_norm, noise_mult):
        n_layers = x_in.shape[0]
        micro, per_micro = d_out.shape[:2]
        examples = micro * per_micro * dp_size
        me = lax.axis_index("tp").astype(jnp.int32)
        my_dp = lax.axis_index("dp").astype(jnp.int32)
        me_arr = me.reshape(1)
        chunks = [(m, e) for m in range(micro) for e in range(0, per_micro, PER_CHUNK)]
        orders = [k % 2 == 0 for k in range(len(chunks))]
        cots = [d_out] * len(chunks)
        pieces = [None] * len(chunks)
        norms = [None] * len(chunks)
        saved = [None] * n_layers
        top = n_layers - 1
        swap_dp = [(i, 1 - i) for i in range(dp_size)]
        ex_all = micro * per_micro
        ex_m, ex_e = me // per_micro, me % per_micro
        cot_slice = lax.dynamic_slice(d_out, (ex_m, ex_e, 0, 0), (1, 1, *d_out.shape[2:]))[0]
        x_slice = lax.dynamic_slice(x_in, (top, ex_m, ex_e, 0, (1 - my_dp) * HALF), (1, 1, 1, d_out.shape[2], HALF))[0, 0]
        cot_other = lax.ppermute(cot_slice, "dp", swap_dp)
        u_other = lax.ppermute(u_pre[top].reshape(ex_all, *u_pre.shape[3:]), "dp", swap_dp)
        x_other = lax.ppermute(x_slice, "dp", swap_dp)
        for layer in reversed(range(n_layers)):
            top = layer == n_layers - 1
            hids, dhids, full = [], [], []
            for k, (m, e) in enumerate(chunks):
                hidden, d_hid, keep, send, norms[k], cot = backward_chunk(
                    layer, m, e, orders[k], me_arr, cots[k], norms[k], x_in, u_pre, w_up, w_down
                )
                if (layer, k) == (0, 1):
                    cot_other, x_other, norms[k] = lax.optimization_barrier((cot_other, x_other, norms[k]))
                pieces[k], cots[k] = sum_over_tp(keep, send, cot if top else pieces[k], orders[k])
                hids.append(hidden)
                dhids.append(d_hid)
                full.append(cot)
            saved[layer] = (tuple(hids), tuple(dhids), d_out if top else tuple(full))
        cot_other = lax.all_gather(cot_other, "tp", axis=0, tiled=True)
        x_other = lax.all_gather(x_other, "tp", axis=0, tiled=True)
        hid_other, dhid_other = hidden_again(n_layers - 1, u_other, cot_other, w_down)
        d_in = join_slots(me_arr, orders, cots, d_out.shape)
        norm_vec = lax.psum(jnp.sum(jnp.concatenate(norms), axis=(1, 2)), "tp")
        clip = jnp.minimum(1.0, clip_norm[0] / jnp.sqrt(norm_vec))
        noise_scale = (noise_mult[0] * clip_norm[0]).reshape(1)
        own_half, other_half = my_dp.reshape(1), (1 - my_dp).reshape(1)
        top = n_layers - 1
        grads = [(up, layer) for layer in reversed(range(top)) for up in (True, False)]

        def own_segs(up, layer):
            hids, dhids, full = saved[layer]
            segs = []
            for k, (m, e) in enumerate(chunks):
                if up:
                    segs.append((PER_CHUNK, (x_in, layer, True, m * per_micro + e), (dhids[k], None, False, 0)))
                elif isinstance(full, tuple):
                    segs.append((PER_CHUNK, (hids[k], None, False, 0), (full[k], None, True, 0)))
                else:
                    segs.append((PER_CHUNK, (hids[k], None, False, 0), (full, None, True, m * per_micro + e)))
            return segs

        def grad(half, clips, segs, *rest):
            return weight_grad(half, clips, segs, *rest)

        def noise_of(up, layer):
            return (noise_up if up else noise_down, layer, noise_scale)

        got = []
        for up, layer in grads:
            part = grad(other_half, clip, own_segs(up, layer))
            got.append(lax.ppermute(part, "dp", swap_dp))
        result = [None, None]
        clip_all = jnp.concatenate([clip, lax.ppermute(clip, "dp", swap_dp)])
        inv = 1.0 / examples
        for up in (True, False):
            rest = ((x_other, None, False, 0), (dhid_other, None, False, 0)) if up else ((hid_other, None, False, 0), (cot_other, None, True, 0))
            segs = own_segs(up, top) + [(ex_all, *rest)]
            result[up] = grad(own_half, clip_all, segs, noise_of(up, top), None, inv, (top, n_layers, None))
        for i, (up, layer) in enumerate(grads):
            last = i == len(grads) - 1
            if last:
                own = grad(own_half, clip, own_segs(up, layer), noise_of(up, layer))
            else:
                result[up] = grad(
                    own_half, clip, own_segs(up, layer), noise_of(up, layer), got[i], inv, (layer, n_layers, result[up])
                )
        own, d_in = lax.optimization_barrier((own, d_in))
        result[up] = finish_grad(layer, n_layers, examples, own, got[-1], result[up])
        return result[1], result[0], d_in

    in_specs = (P(None, None, "dp", None, None), P(None, None, "dp", None, "tp"), P(None, None, "tp"), P(None, "tp", None), P(None, "dp", None, None), P(None, "dp", "tp"), P(None, "tp", "dp"), P(), P())
    out_specs = (P(None, "dp", "tp"), P(None, "tp", "dp"), P(None, "dp", None, None))
    return jax.shard_map(local_pass, mesh=mesh, in_specs=in_specs, out_specs=out_specs, check_vma=False)
```

```python
import functools
import math

import jax
import jax.numpy as jnp
from jax import lax
from jax.experimental import pallas as pl
from jax.experimental.pallas import tpu as pltpu
from jax.sharding import PartitionSpec as P


PIECE = 256
HALF = 1024
PER_CHUNK = 2
TANH_SCALE = math.sqrt(2.0 / math.pi)
TANH_CUBE = 0.044715

NT = (((1,), (1,)), ((), ()))
TN = (((0,), (0,)), ((), ()))


def dot(lhs, rhs, dims):
    return lax.dot_general(lhs, rhs, dims, preferred_element_type=jnp.float32)


def piece_of(me, r1, r2, rc, x_first):
    bits = (r2 * 4 + r1 * 2 + rc) if x_first else (r1 * 4 + r2 * 2 + rc)
    return me ^ bits


def hidden_of(u_ref, cot, w2, h_ref, dh_ref, before=lambda j: None):
    width = 256
    for j in range(u_ref.shape[-1] // width):
        before(j)
        cols = slice(j * width, (j + 1) * width)
        d_act = dot(cot[...], w2[cols, :], NT)
        u = u_ref[:, cols].astype(jnp.float32)
        u_sq = u * u
        t = jnp.tanh(TANH_SCALE * (u + TANH_CUBE * (u_sq * u)))
        cdf = 0.5 * (1.0 + t)
        slope = cdf + (0.5 * TANH_SCALE) * (1.0 - t * t) * (u * (1.0 + (3.0 * TANH_CUBE) * u_sq))
        h_ref[:, cols] = (u * cdf).astype(jnp.bfloat16)
        dh_ref[:, cols] = (slope * d_act).astype(jnp.bfloat16)


def gram_product(left, right):
    prod = dot(left[...], left[:256, :], NT) * dot(right[...], right[:256, :], NT)
    corner = dot(left[256:, :], left[256:, :], NT) * dot(right[256:, :], right[256:, :], NT)
    total = prod[:256] + 2.0 * prod[256:] + corner
    return jnp.sum(total.reshape(32, 8, 256), axis=0)


def backward_kernel(layer, micro, first_ex, x_first, from_slots, do_back, me_ref, *refs):
    refs = list(refs)
    slot_refs = [refs.pop(0) for _ in range(4 if from_slots else 1)]
    u_ref, w2_hbm, last_hbm, h_ref, dh_ref, dz_ref = refs[:6]
    me = me_ref[0]
    step = pl.program_id(0)
    slots = [(rc, r1, r2) for rc in (1, 0) for r1 in range(2) for r2 in range(2)]
    hid = u_ref.shape[-1]
    if do_back:
        keep_ref, send_ref, w2, w2_sem, w1, w1_sem = refs[6:]
    else:
        norm_ref, w2, w2_sem, x_buf, x_sem = refs[6:]

    def rows_of(rc, r1, r2):
        return pl.ds(pl.multiple_of(piece_of(me, r1, r2, rc, x_first) * PIECE, PIECE), PIECE)

    def w2_copy(i):
        rows = pl.ds(i * (hid // 2), hid // 2)
        return pltpu.make_async_copy(w2_hbm.at[layer, rows, :], w2.at[rows, :], w2_sem.at[i])

    def w1_copy(i):
        return pltpu.make_async_copy(last_hbm.at[layer, rows_of(*slots[i]), :], w1.at[i], w1_sem.at[i])

    def x_copy():
        return pltpu.make_async_copy(last_hbm.at[layer, micro, first_ex + step], x_buf, x_sem)

    @pl.when(step == 0)
    def _():
        for i in range(2):
            w2_copy(i).start()
        if do_back:
            for i in range(8):
                w1_copy(i).start()

    if not do_back:
        x_copy().start()
    if from_slots:
        own, first, core_own, core_first = slot_refs
        for rc, r1, slot in ((0, 0, own), (0, 1, first), (1, 0, core_own), (1, 1, core_first)):
            for r2 in range(2):
                dz_ref[:, rows_of(rc, r1, r2)] = slot[r2]
        cot = dz_ref
    else:
        cot = slot_refs[0]
        dz_ref[...] = cot[:, pl.ds(pl.multiple_of(me * PIECE, PIECE), PIECE)]

    def wait_weights(j):
        if j % 2 == 0:

            @pl.when(step == 0)
            def _():
                w2_copy(j // 2).wait()

    hidden_of(u_ref, cot, w2, h_ref, dh_ref, wait_weights)
    if do_back:

        @pl.when(step == 0)
        def _():
            for i in range(8):
                w1_copy(i).wait()

        for i, (rc, r1, r2) in enumerate(slots):
            out = send_ref if rc else keep_ref
            out[r1, r2] = dot(dh_ref[...], w1[i], NT).astype(jnp.bfloat16)
    else:
        norm = gram_product(h_ref, cot)
        x_copy().wait()
        norm_ref[...] = norm + gram_product(dh_ref, x_buf)


NORM_SPEC = pl.BlockSpec((None, 8, 256), lambda e, *_: (e, 0, 0))
NORM_SHAPE = jax.ShapeDtypeStruct((PER_CHUNK, 8, 256), jnp.float32)
PART_SPEC = pl.BlockSpec((2, 2, 512, PIECE), lambda e, *_: (0, 0, e, 0))
PART_SHAPE = jax.ShapeDtypeStruct((2, 2, PER_CHUNK * 512, PIECE), jnp.bfloat16)
ANY_SPEC = pl.BlockSpec(memory_space=pl.ANY)


def backward_chunk(layer, micro, first_ex, x_first, me, dz_inputs, do_back, x_in, u_pre, w_up, w_down):
    rows = PER_CHUNK * 512
    hid, model = u_pre.shape[-1], w_up.shape[1]
    from_slots = isinstance(dz_inputs, tuple)
    if from_slots:
        in_specs = [pl.BlockSpec((2, 512, PIECE), lambda e, m: (0, e, 0))] * 4
    else:
        in_specs = [pl.BlockSpec((None, None, 512, model), lambda e, m: (micro, first_ex + e, 0, 0))]
        dz_inputs = (dz_inputs,)
    act_spec = pl.BlockSpec((512, hid), lambda e, m: (e, 0))
    act_shape = jax.ShapeDtypeStruct((rows, hid), jnp.bfloat16)
    dz_cols = model if from_slots else PIECE
    if do_back:
        last_specs, last_shapes = [PART_SPEC] * 2, [PART_SHAPE] * 2
        scratch = [pltpu.VMEM((8, PIECE, hid), jnp.bfloat16), pltpu.SemaphoreType.DMA((8,))]
    else:
        last_specs, last_shapes = [NORM_SPEC], [NORM_SHAPE]
        scratch = [pltpu.VMEM((512, model), jnp.bfloat16), pltpu.SemaphoreType.DMA]
    return pl.pallas_call(
        functools.partial(backward_kernel, layer, micro, first_ex, x_first, from_slots, do_back),
        grid_spec=pltpu.PrefetchScalarGridSpec(
            num_scalar_prefetch=1,
            grid=(PER_CHUNK,),
            in_specs=in_specs
            + [pl.BlockSpec((None, None, None, 512, hid), lambda e, m: (layer, micro, first_ex + e, 0, 0))]
            + [ANY_SPEC] * 2,
            out_specs=[act_spec, act_spec, pl.BlockSpec((512, dz_cols), lambda e, m: (e, 0))] + last_specs,
            scratch_shapes=[pltpu.VMEM((hid, model), jnp.bfloat16), pltpu.SemaphoreType.DMA((2,))] + scratch,
        ),
        out_shape=[act_shape, act_shape, jax.ShapeDtypeStruct((rows, dz_cols), jnp.bfloat16)] + last_shapes,
        compiler_params=pltpu.CompilerParams(dimension_semantics=("arbitrary",)),
        cost_estimate=pl.CostEstimate(flops=4 * rows * hid * model, bytes_accessed=24 << 20, transcendentals=rows * hid),
    )(me, *dz_inputs, u_pre, w_down, w_up if do_back else x_in)


def norm_kernel(h_ref, dh_ref, dz_ref, x_ref, out_ref):
    out_ref[...] = gram_product(h_ref, dz_ref) + gram_product(dh_ref, x_ref)


def norm_chunk(layer, micro, first_ex, hidden, d_hid, cot, x_in):
    hid, model = hidden.shape[1], x_in.shape[-1]
    act_spec = pl.BlockSpec((512, hid), lambda e: (e, 0))
    if cot.ndim == 4:
        cot_spec = pl.BlockSpec((None, None, 512, model), lambda e: (micro, first_ex + e, 0, 0))
    else:
        cot_spec = pl.BlockSpec((512, model), lambda e: (e, 0))
    x_spec = pl.BlockSpec((None, None, None, 512, model), lambda e: (layer, micro, first_ex + e, 0, 0))
    return pl.pallas_call(
        norm_kernel,
        grid=(PER_CHUNK,),
        in_specs=[act_spec, act_spec, cot_spec, x_spec],
        out_specs=NORM_SPEC,
        out_shape=NORM_SHAPE,
        compiler_params=pltpu.CompilerParams(dimension_semantics=("arbitrary",)),
        cost_estimate=pl.CostEstimate(flops=3 * PER_CHUNK * 512 * 512 * (hid + model), bytes_accessed=12 << 20, transcendentals=0),
    )(hidden, d_hid, cot, x_in)


def back_kernel(x_first, me_ref, dh_ref, w1_ref, keep_ref, send_ref):
    for rc, out in ((1, send_ref), (0, keep_ref)):
        for r1 in range(2):
            for r2 in range(2):
                start = pl.multiple_of(piece_of(me_ref[0], r1, r2, rc, x_first) * PIECE, PIECE)
                out[r1, r2] = dot(dh_ref[...], w1_ref[pl.ds(start, PIECE), :], NT).astype(jnp.bfloat16)


def back_chunk(layer, x_first, me, d_hid, w_up):
    rows, hid = d_hid.shape
    model = w_up.shape[1]
    return pl.pallas_call(
        functools.partial(back_kernel, x_first),
        grid_spec=pltpu.PrefetchScalarGridSpec(
            num_scalar_prefetch=1,
            grid=(PER_CHUNK,),
            in_specs=[
                pl.BlockSpec((512, hid), lambda e, m: (e, 0)),
                pl.BlockSpec((None, model, hid), lambda e, m: (layer, 0, 0)),
            ],
            out_specs=[PART_SPEC] * 2,
        ),
        out_shape=[PART_SHAPE] * 2,
        compiler_params=pltpu.CompilerParams(dimension_semantics=("arbitrary",)),
        cost_estimate=pl.CostEstimate(flops=2 * rows * hid * model, bytes_accessed=10 << 20, transcendentals=0),
        name="back_chunk",
    )(me, d_hid, w_up)


def grad_kernel(segs, n_lhs, n_rhs, init_layer, has_init, has_got, inv, half_ref, clip_ref, *refs):
    refs = list(refs)
    scale_ref = refs.pop(0) if has_init else None
    lhs = [refs.pop(0) for _ in range(n_lhs)]
    rhs = [refs.pop(0) for _ in range(n_rhs)]
    init = refs.pop(0) if has_init else None
    got = refs.pop(0) if has_got else None
    out_ref, a_buf, b_buf, a_sem, b_sem, *extra = refs[-5 - 2 * (has_init + has_got) :]
    init_buf, init_sem = extra[:2] if has_init else (None, None)
    got_buf, got_sem = extra[-2:] if has_got else (None, None)
    half = half_ref[0]
    step = pl.program_id(0)
    n_steps = pl.num_programs(0)

    def view(ref, kind, e):
        layer, cols = kind
        cols = pl.ds(pl.multiple_of(half * HALF, HALF), HALF) if cols else pl.ds(0, 1024)
        if layer is not None:
            return ref.at[layer, e // 4, e % 4, :, cols]
        if len(ref.shape) == 4:
            return ref.at[e // 4, e % 4, :, cols]
        if len(ref.shape) == 3:
            return ref.at[e, :, cols]
        return ref.at[pl.ds(pl.multiple_of(e * 512, 512), 512), cols]

    def fetch(at, slot):
        for start, count, left, left_kind, left_first, right, right_kind, right_first in segs:

            @pl.when(jnp.logical_and(at >= start, at < start + count))
            def _():
                e = at - start
                pltpu.make_async_copy(view(lhs[left], left_kind, e + left_first), a_buf.at[slot], a_sem.at[slot]).start()
                pltpu.make_async_copy(view(rhs[right], right_kind, e + right_first), b_buf.at[slot], b_sem.at[slot]).start()

    slot = step % 2

    @pl.when(step == 0)
    def _():
        fetch(0, 0)
        out_ref[...] = jnp.zeros_like(out_ref)

    @pl.when(step + 1 < n_steps)
    def _():
        fetch(step + 1, 1 - slot)

    @pl.when(step == 1)
    def _():
        if has_init:
            pltpu.make_async_copy(init.at[init_layer], init_buf, init_sem).start()
        if has_got:
            pltpu.make_async_copy(got, got_buf, got_sem).start()

    pltpu.make_async_copy(a_buf.at[slot], a_buf.at[slot], a_sem.at[slot]).wait()
    pltpu.make_async_copy(b_buf.at[slot], b_buf.at[slot], b_sem.at[slot]).wait()
    scaled = (b_buf[slot].astype(jnp.float32) * clip_ref[step]).astype(jnp.bfloat16)
    for j in range(2):
        cols = slice(j * 512, (j + 1) * 512)
        out_ref[:, cols] += dot(a_buf[slot], scaled[:, cols], TN)

    if has_init or has_got:

        @pl.when(step == n_steps - 1)
        def _():
            total = out_ref[...]
            if has_init:
                pltpu.make_async_copy(init.at[init_layer], init_buf, init_sem).wait()
                total = total + scale_ref[0] * init_buf[...]
            if has_got:
                pltpu.make_async_copy(got, got_buf, got_sem).wait()
                total = total + got_buf[...]
            out_ref[...] = total * inv if inv is not None else total


def weight_grad(half, clip, segs, init=None, got=None, inv=None, result=None):
    lhs, rhs, table, at = [], [], [], 0

    def place(group, value):
        for i, other in enumerate(group):
            if other is value:
                return i
        group.append(value)
        return len(group) - 1

    for count, (a, a_layer, a_half, a_first), (b, b_layer, b_half, b_first) in segs:
        left, right = place(lhs, a), place(rhs, b)
        table.append((at, count, left, (a_layer, a_half), a_first, right, (b_layer, b_half), b_first))
        at += count
    any_spec = pl.BlockSpec(memory_space=pl.ANY)
    smem_spec = pl.BlockSpec(memory_space=pltpu.SMEM)
    operands, in_specs = [clip], [smem_spec]
    scratch = [
        pltpu.VMEM((2, 512, 1024), jnp.bfloat16),
        pltpu.VMEM((2, 512, 1024), jnp.bfloat16),
        pltpu.SemaphoreType.DMA((2,)),
        pltpu.SemaphoreType.DMA((2,)),
    ]
    if init is not None:
        operands.append(init[2])
        in_specs.append(smem_spec)
    operands += lhs + rhs
    in_specs += [any_spec] * (len(lhs) + len(rhs))
    for value in (init[0] if init is not None else None, got):
        if value is not None:
            operands.append(value)
            in_specs.append(any_spec)
            scratch += [pltpu.VMEM((1024, 1024), jnp.float32), pltpu.SemaphoreType.DMA]
    aliases = {}
    out_spec, out_shape = pl.BlockSpec((1024, 1024), lambda s, h: (0, 0)), (1024, 1024)
    if result is not None:
        out_layer, n_layers, buffer = result
        out_spec, out_shape = pl.BlockSpec((None, 1024, 1024), lambda s, h: (out_layer, 0, 0)), (n_layers, 1024, 1024)
        if buffer is not None:
            aliases = {len(operands) + 1: 0}
            operands.append(buffer)
            in_specs.append(any_spec)
    return pl.pallas_call(
        functools.partial(
            grad_kernel, table, len(lhs), len(rhs), init[1] if init is not None else 0, init is not None, got is not None, inv
        ),
        grid_spec=pltpu.PrefetchScalarGridSpec(
            num_scalar_prefetch=1, grid=(at,), in_specs=in_specs, out_specs=out_spec, scratch_shapes=scratch
        ),
        out_shape=jax.ShapeDtypeStruct(out_shape, jnp.float32),
        input_output_aliases=aliases,
        compiler_params=pltpu.CompilerParams(dimension_semantics=("arbitrary",)),
        cost_estimate=pl.CostEstimate(flops=2 * at * 512 * 1024 * 1024, bytes_accessed=24 << 20, transcendentals=0),
    )(half, *operands)


def hidden_kernel(from_ref, u_ref, dz_ref, w2_ref, h_ref, dh_ref):
    hidden_of(u_ref, dz_ref, w2_ref, h_ref, dh_ref)


def hidden_again(layer, from_micro, u_other, cot_other, w_down):
    n_ex, _, model = cot_other.shape
    hid = u_other.shape[-1]
    act_spec = pl.BlockSpec((512, hid), lambda e, m: (e, 0))
    act_shape = jax.ShapeDtypeStruct((n_ex * 512, hid), jnp.bfloat16)
    return pl.pallas_call(
        hidden_kernel,
        grid_spec=pltpu.PrefetchScalarGridSpec(
            num_scalar_prefetch=1,
            grid=(n_ex,),
            in_specs=[
                pl.BlockSpec((None, None, 512, hid), lambda e, m: (m[0], e, 0, 0)),
                pl.BlockSpec((None, 512, model), lambda e, m: (e, 0, 0)),
                pl.BlockSpec((None, hid, model), lambda e, m: (layer, 0, 0)),
            ],
            out_specs=[act_spec, act_spec],
        ),
        out_shape=[act_shape, act_shape],
        compiler_params=pltpu.CompilerParams(dimension_semantics=("arbitrary",)),
        cost_estimate=pl.CostEstimate(flops=2 * n_ex * 512 * hid * model, bytes_accessed=24 << 20, transcendentals=n_ex * 512 * hid),
        name="hidden_again",
    )(from_micro, u_other, cot_other, w_down)


def finish_kernel(inv, has_got, own_ref, *refs):
    total = own_ref[...] + refs[0][...] if has_got else own_ref[...]
    refs[-1][...] = total * inv


def finish_grad(layer, n_layers, examples, own, got, buffer):
    spec = pl.BlockSpec((256, 1024), lambda i: (i, 0))
    operands = (own,) if got is None else (own, got)
    in_specs, aliases = [spec] * len(operands), {}
    if buffer is not None:
        aliases = {len(operands): 0}
        operands += (buffer,)
        in_specs.append(pl.BlockSpec(memory_space=pl.ANY))
    return pl.pallas_call(
        functools.partial(finish_kernel, 1.0 / examples, got is not None),
        grid=(4,),
        in_specs=in_specs,
        out_specs=pl.BlockSpec((None, 256, 1024), lambda i: (layer, i, 0)),
        out_shape=jax.ShapeDtypeStruct((n_layers, 1024, 1024), jnp.float32),
        input_output_aliases=aliases,
        compiler_params=pltpu.CompilerParams(dimension_semantics=("arbitrary",)),
        cost_estimate=pl.CostEstimate(flops=12 << 20, bytes_accessed=12 << 20, transcendentals=0),
    )(*operands)


def join_kernel(orders, me_ref, *refs):
    out_ref = refs[-1]
    step = pl.program_id(0)
    for k, x_first in enumerate(orders):

        @pl.when(step // PER_CHUNK == k)
        def _(k=k, x_first=x_first):
            own, first, core_own, core_first = refs[4 * k : 4 * k + 4]
            for rc, r1, slots in ((0, 0, own), (0, 1, first), (1, 0, core_own), (1, 1, core_first)):
                for r2 in range(2):
                    start = pl.multiple_of(piece_of(me_ref[0], r1, r2, rc, x_first) * PIECE, PIECE)
                    out_ref[:, pl.ds(start, PIECE)] = slots[r2]


def join_slots(me, orders, chunks, shape):
    def spec(k):
        return pl.BlockSpec((2, 512, PIECE), lambda s, m: (0, jnp.clip(s - PER_CHUNK * k, 0, PER_CHUNK - 1), 0))

    return pl.pallas_call(
        functools.partial(join_kernel, orders),
        grid_spec=pltpu.PrefetchScalarGridSpec(
            num_scalar_prefetch=1,
            grid=(len(orders) * PER_CHUNK,),
            in_specs=[spec(k) for k in range(len(orders)) for _ in range(4)],
            out_specs=pl.BlockSpec((None, None, 512, shape[-1]), lambda s, m: (s // 4, s % 4, 0, 0)),
        ),
        out_shape=jax.ShapeDtypeStruct(shape, jnp.bfloat16),
        compiler_params=pltpu.CompilerParams(dimension_semantics=("arbitrary",)),
        cost_estimate=pl.CostEstimate(flops=32 << 20, bytes_accessed=32 << 20, transcendentals=0),
        name="join_d_in",
    )(me, *[s for chunk in chunks for s in chunk])


def solution(mesh):
    dp_size, tp_size = mesh.shape["dp"], mesh.shape["tp"]
    CORE, X, Y = 1, 2, 4

    def swap(value, mask):
        return lax.ppermute(value, "tp", [(i, i ^ mask) for i in range(tp_size)])

    def add(a, b):
        return (a.astype(jnp.float32) + b.astype(jnp.float32)).astype(jnp.bfloat16)

    def sum_over_tp(keep, send, cot_piece, x_first):
        one, two = (X, Y) if x_first else (Y, X)
        got = swap(send, CORE)
        away, kept = add(keep[1], got[1]), add(keep[0], got[0])
        got = swap(away, one)
        away = add(kept[1], got[1])
        last = swap(away, two)
        mine = add(kept[0], got[0]).astype(jnp.float32) + last.astype(jnp.float32)
        piece = (cot_piece.astype(jnp.float32) + mine).astype(jnp.bfloat16)
        other = swap(piece, two)
        own = jnp.stack([piece, other])
        first = swap(own, one)
        core_own = swap(own, CORE)
        core_first = swap(first, CORE)
        return piece, (own, first, core_own, core_first)

    def local_pass(x_in, u_pre, w_up, w_down, d_out, noise_up, noise_down, clip_norm, noise_mult):
        n_layers = x_in.shape[0]
        micro, per_micro = d_out.shape[:2]
        examples = micro * per_micro * dp_size
        me = lax.axis_index("tp").astype(jnp.int32)
        my_dp = lax.axis_index("dp").astype(jnp.int32)
        me_arr = me.reshape(1)
        chunks = [(m, e) for m in range(micro) for e in range(0, per_micro, PER_CHUNK)]
        orders = [k % 2 == 0 for k in range(len(chunks))]
        cots = [d_out] * len(chunks)
        pieces = [None] * len(chunks)
        norms = [[] for _ in chunks]
        saved = [None] * n_layers
        top = n_layers - 1
        swap_dp = [(i, 1 - i) for i in range(dp_size)]
        my_core = me % 2
        ex_all = micro * per_micro
        u_other = lax.ppermute(u_pre[top], "dp", swap_dp)
        cot_other = lax.ppermute(lax.dynamic_index_in_dim(d_out, my_core, 0, keepdims=False), "dp", swap_dp)
        x_sizes = (1, 1, *x_in.shape[2:4], HALF)
        x_other = lax.dynamic_slice(x_in, (top, my_core, 0, 0, (1 - my_dp) * HALF), x_sizes)[0, 0]
        x_other = lax.ppermute(x_other, "dp", swap_dp)
        cot_other = (cot_other, swap(cot_other, CORE))
        for layer in reversed(range(n_layers)):
            on_top = layer == top
            hids, dhids, full = [], [], []
            for k, (m, e) in enumerate(chunks):
                hidden, d_hid, cot, *rest = backward_chunk(
                    layer, m, e, orders[k], me_arr, cots[k], layer > 0, x_in, u_pre, w_up, w_down
                )
                if layer > 0:
                    norms[k].append(norm_chunk(layer, m, e, hidden, d_hid, d_out if on_top else cot, x_in))
                    pieces[k], cots[k] = sum_over_tp(*rest, cot if on_top else pieces[k], orders[k])
                else:
                    norms[k].append(rest[0])
                hids.append(hidden)
                dhids.append(d_hid)
                full.append(cot)
            saved[layer] = (tuple(hids), tuple(dhids), d_out if on_top else tuple(full))
        norm_part = sum(jnp.concatenate([norms[k][i] for k in range(len(chunks))]) for i in range(n_layers))
        norm_vec = lax.psum(jnp.sum(norm_part, axis=(1, 2)), "tp")
        clip = jnp.minimum(1.0, clip_norm[0] / jnp.sqrt(norm_vec))
        clip_other = lax.ppermute(clip, "dp", swap_dp)
        for k in range(len(chunks)):
            keep, send = back_chunk(0, orders[k], me_arr, dhids[k], w_up)
            _, cots[k] = sum_over_tp(keep, send, pieces[k], orders[k])
        hid_other, dhid_other = [], []
        for i in range(2):
            h_i, dh_i = hidden_again(top, (my_core ^ i).reshape(1), u_other, cot_other[i], w_down)
            hid_other.append(h_i)
            dhid_other.append(dh_i)
        x_other, clip_other, *hid_other = lax.optimization_barrier((x_other, clip_other, *hid_other))
        x_other = (x_other, swap(x_other, CORE))
        clip_other = lax.dynamic_slice(jnp.concatenate([clip_other, clip_other]), (my_core * per_micro,), (ex_all,))
        clip_all = jnp.concatenate([clip, clip_other])
        d_in = join_slots(me_arr, orders, cots, d_out.shape)
        noise_scale = (noise_mult[0] * clip_norm[0]).reshape(1)
        own_half, other_half = my_dp.reshape(1), (1 - my_dp).reshape(1)
        top = n_layers - 1
        grads = [(up, layer) for layer in reversed(range(top)) for up in (True, False)]

        def own_segs(up, layer):
            hids, dhids, full = saved[layer]
            segs = []
            for k, (m, e) in enumerate(chunks):
                if up:
                    segs.append((PER_CHUNK, (x_in, layer, True, m * per_micro + e), (dhids[k], None, False, 0)))
                elif isinstance(full, tuple):
                    segs.append((PER_CHUNK, (hids[k], None, False, 0), (full[k], None, True, 0)))
                else:
                    segs.append((PER_CHUNK, (hids[k], None, False, 0), (full, None, True, m * per_micro + e)))
            return segs

        def grad(half, clips, segs, *rest):
            return weight_grad(half, clips, segs, *rest)

        def noise_of(up, layer):
            return (noise_up if up else noise_down, layer, noise_scale)

        got = []
        for up, layer in grads:
            part = grad(other_half, clip, own_segs(up, layer))
            got.append(lax.ppermute(part, "dp", swap_dp))
        result = [None, None]
        inv = 1.0 / examples
        for up in (True, False):
            if up:
                rest = [(per_micro, (x_other[r], None, False, 0), (dhid_other[r], None, False, 0)) for r in range(2)]
            else:
                rest = [(per_micro, (hid_other[r], None, False, 0), (cot_other[r], None, True, 0)) for r in range(2)]
            segs = own_segs(up, top) + rest
            result[up] = grad(own_half, clip_all, segs, noise_of(up, top), None, inv, (top, n_layers, None))
        for i, (up, layer) in enumerate(grads):
            last = i == len(grads) - 1
            if last:
                own = grad(own_half, clip, own_segs(up, layer), noise_of(up, layer))
            else:
                result[up] = grad(
                    own_half, clip, own_segs(up, layer), noise_of(up, layer), got[i], inv, (layer, n_layers, result[up])
                )
        own, d_in = lax.optimization_barrier((own, d_in))
        result[up] = finish_grad(layer, n_layers, examples, own, got[-1], result[up])
        return result[1], result[0], d_in

    in_specs = (P(None, None, "dp", None, None), P(None, None, "dp", None, "tp"), P(None, None, "tp"), P(None, "tp", None), P(None, "dp", None, None), P(None, "dp", "tp"), P(None, "tp", "dp"), P(), P())
    out_specs = (P(None, "dp", "tp"), P(None, "tp", "dp"), P(None, "dp", None, None))
    return jax.shard_map(local_pass, mesh=mesh, in_specs=in_specs, out_specs=out_specs, check_vma=False)
```

```python
import functools
import math

import jax
import jax.numpy as jnp
from jax import lax
from jax.experimental import pallas as pl
from jax.experimental.pallas import tpu as pltpu
from jax.sharding import PartitionSpec as P


PIECE = 256
HALF = 1024
PER_CHUNK = 2
ROWS = 512
WIDE = 1024
BLOCK = 256
TANH_SCALE = math.sqrt(2.0 / math.pi)
TANH_CUBE = 0.044715

NT = (((1,), (1,)), ((), ()))
TN = (((0,), (0,)), ((), ()))


def dot(lhs, rhs, dims):
    return lax.dot_general(lhs, rhs, dims, preferred_element_type=jnp.float32)


def piece_of(me, r1, r2, rc, x_first):
    bits = (r2 * 4 + r1 * 2 + rc) if x_first else (r1 * 4 + r2 * 2 + rc)
    return me ^ bits


def hidden_of(u_ref, cot, w2, h_ref, dh_ref, before=lambda j: None):
    width = BLOCK
    for j in range(u_ref.shape[-1] // width):
        before(j)
        cols = slice(j * width, (j + 1) * width)
        d_act = dot(cot[...], w2[cols, :], NT)
        u = u_ref[:, cols].astype(jnp.float32)
        u_sq = u * u
        t = jnp.tanh(TANH_SCALE * (u + TANH_CUBE * (u_sq * u)))
        cdf = 0.5 * (1.0 + t)
        slope = cdf + (0.5 * TANH_SCALE) * (1.0 - t * t) * (u * (1.0 + (3.0 * TANH_CUBE) * u_sq))
        h_ref[:, cols] = (u * cdf).astype(jnp.bfloat16)
        dh_ref[:, cols] = (slope * d_act).astype(jnp.bfloat16)


def gram_product(left, right):
    prod = dot(left[...], left[:BLOCK, :], NT) * dot(right[...], right[:BLOCK, :], NT)
    corner = dot(left[BLOCK:, :], left[BLOCK:, :], NT) * dot(right[BLOCK:, :], right[BLOCK:, :], NT)
    total = prod[:BLOCK] + 2.0 * prod[BLOCK:] + corner
    return jnp.sum(total.reshape(32, 8, BLOCK), axis=0)


def backward_kernel(layer, micro, first_ex, x_first, from_slots, do_back, me_ref, *refs):
    refs = list(refs)
    slot_refs = [refs.pop(0) for _ in range(4 if from_slots else 1)]
    u_ref, w2_hbm, last_hbm, h_ref, dh_ref, dz_ref = refs[:6]
    me = me_ref[0]
    step = pl.program_id(0)
    slots = [(rc, r1, r2) for rc in (1, 0) for r1 in range(2) for r2 in range(2)]
    hid = u_ref.shape[-1]
    if do_back:
        keep_ref, send_ref, w2, w2_sem, w1, w1_sem = refs[6:]
    else:
        norm_ref, w2, w2_sem, x_buf, x_sem = refs[6:]

    def rows_of(rc, r1, r2):
        return pl.ds(pl.multiple_of(piece_of(me, r1, r2, rc, x_first) * PIECE, PIECE), PIECE)

    def w2_copy(i):
        rows = pl.ds(i * (hid // 2), hid // 2)
        return pltpu.make_async_copy(w2_hbm.at[layer, rows, :], w2.at[rows, :], w2_sem.at[i])

    def w1_copy(i):
        return pltpu.make_async_copy(last_hbm.at[layer, rows_of(*slots[i]), :], w1.at[i], w1_sem.at[i])

    def x_copy():
        return pltpu.make_async_copy(last_hbm.at[layer, micro, first_ex + step], x_buf, x_sem)

    @pl.when(step == 0)
    def _():
        for i in range(2):
            w2_copy(i).start()

    if not do_back:
        x_copy().start()
    if from_slots:
        own, first, core_own, core_first = slot_refs
        for rc, r1, slot in ((0, 0, own), (0, 1, first), (1, 0, core_own), (1, 1, core_first)):
            for r2 in range(2):
                dz_ref[:, rows_of(rc, r1, r2)] = slot[r2]
        cot = dz_ref
    else:
        cot = slot_refs[0]
        dz_ref[...] = cot[:, pl.ds(pl.multiple_of(me * PIECE, PIECE), PIECE)]

    def wait_weights(j):
        if j % 2 == 0:

            @pl.when(step == 0)
            def _():
                w2_copy(j // 2).wait()
                if do_back and j == 0:
                    for i in range(8):
                        w1_copy(i).start()

    hidden_of(u_ref, cot, w2, h_ref, dh_ref, wait_weights)
    if do_back:

        @pl.when(step == 0)
        def _():
            for i in range(8):
                w1_copy(i).wait()

        for i, (rc, r1, r2) in enumerate(slots):
            out = send_ref if rc else keep_ref
            out[r1, r2] = dot(dh_ref[...], w1[i], NT).astype(jnp.bfloat16)
    else:
        norm = gram_product(h_ref, cot)
        x_copy().wait()
        norm_ref[...] = norm + gram_product(dh_ref, x_buf)


NORM_SPEC = pl.BlockSpec((None, 8, BLOCK), lambda e, *_: (e, 0, 0))
NORM_SHAPE = jax.ShapeDtypeStruct((PER_CHUNK, 8, BLOCK), jnp.float32)
PART_SPEC = pl.BlockSpec((2, 2, ROWS, PIECE), lambda e, *_: (0, 0, e, 0))
PART_SHAPE = jax.ShapeDtypeStruct((2, 2, PER_CHUNK * ROWS, PIECE), jnp.bfloat16)
ANY_SPEC = pl.BlockSpec(memory_space=pl.ANY)


def backward_chunk(layer, micro, first_ex, x_first, me, dz_inputs, do_back, x_in, u_pre, w_up, w_down):
    rows = PER_CHUNK * ROWS
    hid, model = u_pre.shape[-1], w_up.shape[1]
    from_slots = isinstance(dz_inputs, tuple)
    if from_slots:
        in_specs = [pl.BlockSpec((2, ROWS, PIECE), lambda e, m: (0, e, 0))] * 4
    else:
        in_specs = [pl.BlockSpec((None, None, ROWS, model), lambda e, m: (micro, first_ex + e, 0, 0))]
        dz_inputs = (dz_inputs,)
    act_spec = pl.BlockSpec((ROWS, hid), lambda e, m: (e, 0))
    act_shape = jax.ShapeDtypeStruct((rows, hid), jnp.bfloat16)
    dz_cols = model if from_slots else PIECE
    if do_back:
        last_specs, last_shapes = [PART_SPEC] * 2, [PART_SHAPE] * 2
        scratch = [pltpu.VMEM((8, PIECE, hid), jnp.bfloat16), pltpu.SemaphoreType.DMA((8,))]
    else:
        last_specs, last_shapes = [NORM_SPEC], [NORM_SHAPE]
        scratch = [pltpu.VMEM((ROWS, model), jnp.bfloat16), pltpu.SemaphoreType.DMA]
    return pl.pallas_call(
        functools.partial(backward_kernel, layer, micro, first_ex, x_first, from_slots, do_back),
        grid_spec=pltpu.PrefetchScalarGridSpec(
            num_scalar_prefetch=1,
            grid=(PER_CHUNK,),
            in_specs=in_specs
            + [pl.BlockSpec((None, None, None, ROWS, hid), lambda e, m: (layer, micro, first_ex + e, 0, 0))]
            + [ANY_SPEC] * 2,
            out_specs=[act_spec, act_spec, pl.BlockSpec((ROWS, dz_cols), lambda e, m: (e, 0))] + last_specs,
            scratch_shapes=[pltpu.VMEM((hid, model), jnp.bfloat16), pltpu.SemaphoreType.DMA((2,))] + scratch,
        ),
        out_shape=[act_shape, act_shape, jax.ShapeDtypeStruct((rows, dz_cols), jnp.bfloat16)] + last_shapes,
        compiler_params=pltpu.CompilerParams(dimension_semantics=("arbitrary",)),
        cost_estimate=pl.CostEstimate(flops=4 * rows * hid * model, bytes_accessed=24 << 20, transcendentals=rows * hid),
    )(me, *dz_inputs, u_pre, w_down, w_up if do_back else x_in)


def norm_kernel(h_ref, dh_ref, dz_ref, x_ref, out_ref):
    out_ref[...] = gram_product(h_ref, dz_ref) + gram_product(dh_ref, x_ref)


def norm_chunk(layer, micro, first_ex, hidden, d_hid, cot, x_in):
    hid, model = hidden.shape[1], x_in.shape[-1]
    act_spec = pl.BlockSpec((ROWS, hid), lambda e: (e, 0))
    if cot.ndim == 4:
        cot_spec = pl.BlockSpec((None, None, ROWS, model), lambda e: (micro, first_ex + e, 0, 0))
    else:
        cot_spec = pl.BlockSpec((ROWS, model), lambda e: (e, 0))
    x_spec = pl.BlockSpec((None, None, None, ROWS, model), lambda e: (layer, micro, first_ex + e, 0, 0))
    return pl.pallas_call(
        norm_kernel,
        grid=(PER_CHUNK,),
        in_specs=[act_spec, act_spec, cot_spec, x_spec],
        out_specs=NORM_SPEC,
        out_shape=NORM_SHAPE,
        compiler_params=pltpu.CompilerParams(dimension_semantics=("arbitrary",)),
        cost_estimate=pl.CostEstimate(flops=3 * PER_CHUNK * ROWS * ROWS * (hid + model), bytes_accessed=12 << 20, transcendentals=0),
    )(hidden, d_hid, cot, x_in)


def back_kernel(x_first, me_ref, dh_ref, w1_ref, keep_ref, send_ref):
    for rc, out in ((1, send_ref), (0, keep_ref)):
        for r1 in range(2):
            for r2 in range(2):
                start = pl.multiple_of(piece_of(me_ref[0], r1, r2, rc, x_first) * PIECE, PIECE)
                out[r1, r2] = dot(dh_ref[...], w1_ref[pl.ds(start, PIECE), :], NT).astype(jnp.bfloat16)


def back_chunk(layer, x_first, me, d_hid, w_up):
    rows, hid = d_hid.shape
    model = w_up.shape[1]
    return pl.pallas_call(
        functools.partial(back_kernel, x_first),
        grid_spec=pltpu.PrefetchScalarGridSpec(
            num_scalar_prefetch=1,
            grid=(PER_CHUNK,),
            in_specs=[
                pl.BlockSpec((ROWS, hid), lambda e, m: (e, 0)),
                pl.BlockSpec((None, model, hid), lambda e, m: (layer, 0, 0)),
            ],
            out_specs=[PART_SPEC] * 2,
        ),
        out_shape=[PART_SHAPE] * 2,
        compiler_params=pltpu.CompilerParams(dimension_semantics=("arbitrary",)),
        cost_estimate=pl.CostEstimate(flops=2 * rows * hid * model, bytes_accessed=10 << 20, transcendentals=0),
        name="back_chunk",
    )(me, d_hid, w_up)


def grad_kernel(segs, n_lhs, n_rhs, init_layer, has_init, has_got, inv, half_ref, clip_ref, *refs):
    refs = list(refs)
    scale_ref = refs.pop(0) if has_init else None
    lhs = [refs.pop(0) for _ in range(n_lhs)]
    rhs = [refs.pop(0) for _ in range(n_rhs)]
    init = refs.pop(0) if has_init else None
    got = refs.pop(0) if has_got else None
    out_ref, a_buf, b_buf, a_sem, b_sem, *extra = refs[-5 - 2 * (has_init + has_got) :]
    init_buf, init_sem = extra[:2] if has_init else (None, None)
    got_buf, got_sem = extra[-2:] if has_got else (None, None)
    half = half_ref[0]
    step = pl.program_id(0)
    n_steps = pl.num_programs(0)

    def view(ref, kind, e):
        layer, cols = kind
        cols = pl.ds(pl.multiple_of(half * HALF, HALF), HALF) if cols else pl.ds(0, WIDE)
        if layer is not None:
            return ref.at[layer, e // 4, e % 4, :, cols]
        if len(ref.shape) == 4:
            return ref.at[e // 4, e % 4, :, cols]
        if len(ref.shape) == 3:
            return ref.at[e, :, cols]
        return ref.at[pl.ds(pl.multiple_of(e * ROWS, ROWS), ROWS), cols]

    def fetch(at, slot):
        for start, count, left, left_kind, left_first, right, right_kind, right_first in segs:

            @pl.when(jnp.logical_and(at >= start, at < start + count))
            def _():
                e = at - start
                pltpu.make_async_copy(view(lhs[left], left_kind, e + left_first), a_buf.at[slot], a_sem.at[slot]).start()
                pltpu.make_async_copy(view(rhs[right], right_kind, e + right_first), b_buf.at[slot], b_sem.at[slot]).start()

    slot = step % 2

    @pl.when(step == 0)
    def _():
        fetch(0, 0)
        out_ref[...] = jnp.zeros_like(out_ref)

    @pl.when(step + 1 < n_steps)
    def _():
        fetch(step + 1, 1 - slot)

    @pl.when(step == 1)
    def _():
        if has_init:
            pltpu.make_async_copy(init.at[init_layer], init_buf, init_sem).start()
        if has_got:
            pltpu.make_async_copy(got, got_buf, got_sem).start()

    pltpu.make_async_copy(a_buf.at[slot], a_buf.at[slot], a_sem.at[slot]).wait()
    pltpu.make_async_copy(b_buf.at[slot], b_buf.at[slot], b_sem.at[slot]).wait()
    scaled = (b_buf[slot].astype(jnp.float32) * clip_ref[step]).astype(jnp.bfloat16)
    for j in range(2):
        cols = slice(j * ROWS, (j + 1) * ROWS)
        out_ref[:, cols] += dot(a_buf[slot], scaled[:, cols], TN)

    if has_init or has_got:

        @pl.when(step == n_steps - 1)
        def _():
            total = out_ref[...]
            if has_init:
                pltpu.make_async_copy(init.at[init_layer], init_buf, init_sem).wait()
                total = total + scale_ref[0] * init_buf[...]
            if has_got:
                pltpu.make_async_copy(got, got_buf, got_sem).wait()
                total = total + got_buf[...]
            out_ref[...] = total * inv if inv is not None else total


def weight_grad(half, clip, segs, init=None, got=None, inv=None, result=None):
    lhs, rhs, table, at = [], [], [], 0

    def place(group, value):
        for i, other in enumerate(group):
            if other is value:
                return i
        group.append(value)
        return len(group) - 1

    for count, (a, a_layer, a_half, a_first), (b, b_layer, b_half, b_first) in segs:
        left, right = place(lhs, a), place(rhs, b)
        table.append((at, count, left, (a_layer, a_half), a_first, right, (b_layer, b_half), b_first))
        at += count
    any_spec = pl.BlockSpec(memory_space=pl.ANY)
    smem_spec = pl.BlockSpec(memory_space=pltpu.SMEM)
    operands, in_specs = [clip], [smem_spec]
    scratch = [
        pltpu.VMEM((2, ROWS, WIDE), jnp.bfloat16),
        pltpu.VMEM((2, ROWS, WIDE), jnp.bfloat16),
        pltpu.SemaphoreType.DMA((2,)),
        pltpu.SemaphoreType.DMA((2,)),
    ]
    if init is not None:
        operands.append(init[2])
        in_specs.append(smem_spec)
    operands += lhs + rhs
    in_specs += [any_spec] * (len(lhs) + len(rhs))
    for value in (init[0] if init is not None else None, got):
        if value is not None:
            operands.append(value)
            in_specs.append(any_spec)
            scratch += [pltpu.VMEM((WIDE, WIDE), jnp.float32), pltpu.SemaphoreType.DMA]
    aliases = {}
    out_spec, out_shape = pl.BlockSpec((WIDE, WIDE), lambda s, h: (0, 0)), (WIDE, WIDE)
    if result is not None:
        out_layer, n_layers, buffer = result
        out_spec, out_shape = pl.BlockSpec((None, WIDE, WIDE), lambda s, h: (out_layer, 0, 0)), (n_layers, WIDE, WIDE)
        if buffer is not None:
            aliases = {len(operands) + 1: 0}
            operands.append(buffer)
            in_specs.append(any_spec)
    return pl.pallas_call(
        functools.partial(
            grad_kernel, table, len(lhs), len(rhs), init[1] if init is not None else 0, init is not None, got is not None, inv
        ),
        grid_spec=pltpu.PrefetchScalarGridSpec(
            num_scalar_prefetch=1, grid=(at,), in_specs=in_specs, out_specs=out_spec, scratch_shapes=scratch
        ),
        out_shape=jax.ShapeDtypeStruct(out_shape, jnp.float32),
        input_output_aliases=aliases,
        compiler_params=pltpu.CompilerParams(dimension_semantics=("arbitrary",)),
        cost_estimate=pl.CostEstimate(flops=2 * at * ROWS * WIDE * WIDE, bytes_accessed=24 << 20, transcendentals=0),
    )(half, *operands)


def hidden_kernel(from_ref, u_ref, dz_ref, w2_ref, h_ref, dh_ref):
    hidden_of(u_ref, dz_ref, w2_ref, h_ref, dh_ref)


def hidden_again(layer, from_micro, u_other, cot_other, w_down):
    n_ex, _, model = cot_other.shape
    hid = u_other.shape[-1]
    act_spec = pl.BlockSpec((ROWS, hid), lambda e, m: (e, 0))
    act_shape = jax.ShapeDtypeStruct((n_ex * ROWS, hid), jnp.bfloat16)
    return pl.pallas_call(
        hidden_kernel,
        grid_spec=pltpu.PrefetchScalarGridSpec(
            num_scalar_prefetch=1,
            grid=(n_ex,),
            in_specs=[
                pl.BlockSpec((None, None, ROWS, hid), lambda e, m: (m[0], e, 0, 0)),
                pl.BlockSpec((None, ROWS, model), lambda e, m: (e, 0, 0)),
                pl.BlockSpec((None, hid, model), lambda e, m: (layer, 0, 0)),
            ],
            out_specs=[act_spec, act_spec],
        ),
        out_shape=[act_shape, act_shape],
        compiler_params=pltpu.CompilerParams(dimension_semantics=("arbitrary",)),
        cost_estimate=pl.CostEstimate(flops=2 * n_ex * ROWS * hid * model, bytes_accessed=24 << 20, transcendentals=n_ex * ROWS * hid),
        name="hidden_again",
    )(from_micro, u_other, cot_other, w_down)


def finish_kernel(inv, has_got, own_ref, *refs):
    total = own_ref[...] + refs[0][...] if has_got else own_ref[...]
    refs[-1][...] = total * inv


def finish_grad(layer, n_layers, examples, own, got, buffer):
    spec = pl.BlockSpec((BLOCK, WIDE), lambda i: (i, 0))
    operands = (own,) if got is None else (own, got)
    in_specs, aliases = [spec] * len(operands), {}
    if buffer is not None:
        aliases = {len(operands): 0}
        operands += (buffer,)
        in_specs.append(pl.BlockSpec(memory_space=pl.ANY))
    return pl.pallas_call(
        functools.partial(finish_kernel, 1.0 / examples, got is not None),
        grid=(4,),
        in_specs=in_specs,
        out_specs=pl.BlockSpec((None, BLOCK, WIDE), lambda i: (layer, i, 0)),
        out_shape=jax.ShapeDtypeStruct((n_layers, WIDE, WIDE), jnp.float32),
        input_output_aliases=aliases,
        compiler_params=pltpu.CompilerParams(dimension_semantics=("arbitrary",)),
        cost_estimate=pl.CostEstimate(flops=12 << 20, bytes_accessed=12 << 20, transcendentals=0),
    )(*operands)


def join_kernel(orders, me_ref, *refs):
    out_ref = refs[-1]
    step = pl.program_id(0)
    for k, x_first in enumerate(orders):

        @pl.when(step // PER_CHUNK == k)
        def _(k=k, x_first=x_first):
            own, first, core_own, core_first = refs[4 * k : 4 * k + 4]
            for rc, r1, slots in ((0, 0, own), (0, 1, first), (1, 0, core_own), (1, 1, core_first)):
                for r2 in range(2):
                    start = pl.multiple_of(piece_of(me_ref[0], r1, r2, rc, x_first) * PIECE, PIECE)
                    out_ref[:, pl.ds(start, PIECE)] = slots[r2]


def join_slots(me, orders, chunks, shape):
    def spec(k):
        return pl.BlockSpec((2, ROWS, PIECE), lambda s, m: (0, jnp.clip(s - PER_CHUNK * k, 0, PER_CHUNK - 1), 0))

    return pl.pallas_call(
        functools.partial(join_kernel, orders),
        grid_spec=pltpu.PrefetchScalarGridSpec(
            num_scalar_prefetch=1,
            grid=(len(orders) * PER_CHUNK,),
            in_specs=[spec(k) for k in range(len(orders)) for _ in range(4)],
            out_specs=pl.BlockSpec((None, None, ROWS, shape[-1]), lambda s, m: (s // 4, s % 4, 0, 0)),
        ),
        out_shape=jax.ShapeDtypeStruct(shape, jnp.bfloat16),
        compiler_params=pltpu.CompilerParams(dimension_semantics=("arbitrary",)),
        cost_estimate=pl.CostEstimate(flops=32 << 20, bytes_accessed=32 << 20, transcendentals=0),
        name="join_d_in",
    )(me, *[s for chunk in chunks for s in chunk])


def solution(mesh):
    dp_size, tp_size = mesh.shape["dp"], mesh.shape["tp"]
    CORE, X, Y = 1, 2, 4

    def swap(value, mask):
        return lax.ppermute(value, "tp", [(i, i ^ mask) for i in range(tp_size)])

    def add(a, b):
        return (a.astype(jnp.float32) + b.astype(jnp.float32)).astype(jnp.bfloat16)

    def sum_over_tp(keep, send, cot_piece, x_first):
        one, two = (X, Y) if x_first else (Y, X)
        got = swap(send, CORE)
        away, kept = add(keep[1], got[1]), add(keep[0], got[0])
        got = swap(away, one)
        away = add(kept[1], got[1])
        last = swap(away, two)
        mine = add(kept[0], got[0]).astype(jnp.float32) + last.astype(jnp.float32)
        piece = (cot_piece.astype(jnp.float32) + mine).astype(jnp.bfloat16)
        other = swap(piece, two)
        own = jnp.stack([piece, other])
        first = swap(own, one)
        core_own = swap(own, CORE)
        core_first = swap(first, CORE)
        return piece, (own, first, core_own, core_first)

    def local_pass(x_in, u_pre, w_up, w_down, d_out, noise_up, noise_down, clip_norm, noise_mult):
        n_layers = x_in.shape[0]
        micro, per_micro = d_out.shape[:2]
        examples = micro * per_micro * dp_size
        me = lax.axis_index("tp").astype(jnp.int32)
        my_dp = lax.axis_index("dp").astype(jnp.int32)
        me_arr = me.reshape(1)
        chunks = [(m, e) for m in range(micro) for e in range(0, per_micro, PER_CHUNK)]
        orders = [k % 2 == 0 for k in range(len(chunks))]
        cots = [d_out] * len(chunks)
        pieces = [None] * len(chunks)
        norms = [[] for _ in chunks]
        saved = [None] * n_layers
        top = n_layers - 1
        swap_dp = [(i, 1 - i) for i in range(dp_size)]
        my_core = me % 2
        ex_all = micro * per_micro
        u_other = lax.ppermute(u_pre[top], "dp", swap_dp)
        cot_other = lax.ppermute(lax.dynamic_index_in_dim(d_out, my_core, 0, keepdims=False), "dp", swap_dp)
        x_sizes = (1, 1, *x_in.shape[2:4], HALF)
        x_other = lax.dynamic_slice(x_in, (top, my_core, 0, 0, (1 - my_dp) * HALF), x_sizes)[0, 0]
        x_other = lax.ppermute(x_other, "dp", swap_dp)
        cot_other = (cot_other, swap(cot_other, CORE))
        for layer in reversed(range(n_layers)):
            on_top = layer == top
            hids, dhids, full = [], [], []
            for k, (m, e) in enumerate(chunks):
                hidden, d_hid, cot, *rest = backward_chunk(
                    layer, m, e, orders[k], me_arr, cots[k], layer > 0, x_in, u_pre, w_up, w_down
                )
                if layer > 0:
                    norms[k].append(norm_chunk(layer, m, e, hidden, d_hid, d_out if on_top else cot, x_in))
                    pieces[k], cots[k] = sum_over_tp(*rest, cot if on_top else pieces[k], orders[k])
                else:
                    norms[k].append(rest[0])
                hids.append(hidden)
                dhids.append(d_hid)
                full.append(cot)
            saved[layer] = (tuple(hids), tuple(dhids), d_out if on_top else tuple(full))
        norm_part = sum(jnp.concatenate([norms[k][i] for k in range(len(chunks))]) for i in range(n_layers))
        norm_vec = lax.psum(jnp.sum(norm_part, axis=(1, 2)), "tp")
        clip = jnp.minimum(1.0, clip_norm[0] / jnp.sqrt(norm_vec))
        clip_other = lax.ppermute(clip, "dp", swap_dp)
        for k in range(len(chunks)):
            keep, send = back_chunk(0, orders[k], me_arr, dhids[k], w_up)
            _, cots[k] = sum_over_tp(keep, send, pieces[k], orders[k])
        hid_other, dhid_other = [], []
        for i in range(2):
            h_i, dh_i = hidden_again(top, (my_core ^ i).reshape(1), u_other, cot_other[i], w_down)
            hid_other.append(h_i)
            dhid_other.append(dh_i)
        x_other, clip_other, *hid_other = lax.optimization_barrier((x_other, clip_other, *hid_other))
        x_other = (x_other, swap(x_other, CORE))
        clip_other = lax.dynamic_slice(jnp.concatenate([clip_other, clip_other]), (my_core * per_micro,), (ex_all,))
        clip_all = jnp.concatenate([clip, clip_other])
        d_in = join_slots(me_arr, orders, cots, d_out.shape)
        noise_scale = (noise_mult[0] * clip_norm[0]).reshape(1)
        own_half, other_half = my_dp.reshape(1), (1 - my_dp).reshape(1)
        top = n_layers - 1
        grads = [(up, layer) for layer in reversed(range(top)) for up in (True, False)]

        def own_segs(up, layer):
            hids, dhids, full = saved[layer]
            segs = []
            for k, (m, e) in enumerate(chunks):
                if up:
                    segs.append((PER_CHUNK, (x_in, layer, True, m * per_micro + e), (dhids[k], None, False, 0)))
                elif isinstance(full, tuple):
                    segs.append((PER_CHUNK, (hids[k], None, False, 0), (full[k], None, True, 0)))
                else:
                    segs.append((PER_CHUNK, (hids[k], None, False, 0), (full, None, True, m * per_micro + e)))
            return segs

        def grad(half, clips, segs, *rest):
            return weight_grad(half, clips, segs, *rest)

        def noise_of(up, layer):
            return (noise_up if up else noise_down, layer, noise_scale)

        got = []
        for up, layer in grads:
            part = grad(other_half, clip, own_segs(up, layer))
            got.append(lax.ppermute(part, "dp", swap_dp))
        result = [None, None]
        inv = 1.0 / examples
        for up in (True, False):
            if up:
                rest = [(per_micro, (x_other[r], None, False, 0), (dhid_other[r], None, False, 0)) for r in range(2)]
            else:
                rest = [(per_micro, (hid_other[r], None, False, 0), (cot_other[r], None, True, 0)) for r in range(2)]
            segs = own_segs(up, top) + rest
            result[up] = grad(own_half, clip_all, segs, noise_of(up, top), None, inv, (top, n_layers, None))
        for i, (up, layer) in enumerate(grads):
            last = i == len(grads) - 1
            if last:
                own = grad(own_half, clip, own_segs(up, layer), noise_of(up, layer))
            else:
                result[up] = grad(
                    own_half, clip, own_segs(up, layer), noise_of(up, layer), got[i], inv, (layer, n_layers, result[up])
                )
        own, d_in = lax.optimization_barrier((own, d_in))
        result[up] = finish_grad(layer, n_layers, examples, own, got[-1], result[up])
        return result[1], result[0], d_in

    in_specs = (P(None, None, "dp", None, None), P(None, None, "dp", None, "tp"), P(None, None, "tp"), P(None, "tp", None), P(None, "dp", None, None), P(None, "dp", "tp"), P(None, "tp", "dp"), P(), P())
    out_specs = (P(None, "dp", "tp"), P(None, "tp", "dp"), P(None, "dp", None, None))
    return jax.shard_map(local_pass, mesh=mesh, in_specs=in_specs, out_specs=out_specs, check_vma=False)
```
